32 devices in a mesh: req: 4 (over z), kvh: 4 (over y, core), exp: 2 (over x).
Axes of the slice: x: 2, y: 2, z: 4, core: 2. Of those that a mesh axis runs over, the one named last changes fastest.
Arguments:
- queries: bfloat16 [512, 2048], P(('req', 'exp'), 'kvh'), may hold values from -170 to 170
- keys: bfloat16 [512, 4, 64, 128], P(('req', 'exp'), 'kvh'), may hold values from -6 to 6
- values: bfloat16 [512, 4, 64, 128], P(('req', 'exp'), 'kvh'), may hold values from -6 to 6
- lengths: int32 [512], P('req'), may hold values from 2 to 64
- out_weight: bfloat16 [2048, 2048], P(('kvh', 'exp')), may hold values from -0.125 to 0.125
- residual: bfloat16 [512, 2048], P('req'), may hold values from -54 to 54
- norm_gain: float32 [2048], replicated, may hold values from 0.5 to 2
- expert_ids: int32 [512, 8], P('req'), may hold values from 0 to 7, as said below
- gate_weights: float32 [512, 8], P('req'), may hold values from 0.2 to 1
- replica_map: int32 [16], replicated, may hold values from 0 to 7, as said below
- w_gate: bfloat16 [16, 2048, 384], P(('req', 'kvh'), None, 'exp')
- w_up: bfloat16 [16, 2048, 384], P(('req', 'kvh'), None, 'exp')
- w_down: bfloat16 [16, 384, 2048], P(('req', 'kvh'), 'exp')
Outputs:
- layer_out: bfloat16 [512, 2048], P('req', ('kvh', 'exp'))
The draws below stay inside these ranges and needn't reach their ends.
Inputs may be any that keep to these rules, and one draw needn't show every extreme that they name: `replica_map`: every one of the 8 experts is served by one or more slots; slots that serve one expert hold equal weights in w_gate, w_up and w_down. `expert_ids`: A token names 8 different experts and every expert is named by some token; among the 128 tokens of one req index no expert is named by more than 128 tokens, and in every req index some expert is named by exactly 128.
All inputs are finite; a program needn't handle non-finite values.
Results may differ from the reference program's by a relative error of at most 0.008.
Values may be sent and summed in bfloat16 or wider, within the bound.
No kernel may reach another device: no remote copies, remote signals or barrier semaphores. Data moves between devices by JAX's collectives and lax.ppermute only.
A program may use at most 64 MiB of HBM per device.

```python
import math
import jax
import jax.numpy as jnp
from jax import lax

D = 2048
HEADS = 16
KVH = 4
HD = 128
HID = 384
TOP = 8
REQ_DEV = 128
CACHE = 64
TOKENS = 512
SLOTS = 16
EXPERTS = 8
MOST = 128
N_REQ = 4


def key_front(key):
    return jnp.clip(jax.random.normal(jax.random.fold_in(key, 102), (TOKENS, KVH, 1, HD), jnp.float32), -6.0, 6.0)


def draw_keys(key, part):
    first = key_front(key)
    rest = jnp.clip(jax.random.normal(jax.random.fold_in(key, 104), (TOKENS, KVH, CACHE - 1, HD), jnp.float32), -6.0, 6.0)
    return jnp.concatenate([first, rest], axis=2).astype(jnp.bfloat16)


def draw_queries(key, part):
    query = jnp.clip(jax.random.normal(jax.random.fold_in(key, 103), (TOKENS, HEADS, HD), jnp.float32), -6.0, 6.0)
    return query.reshape(TOKENS, HEADS * HD).astype(jnp.bfloat16)


def draw_residual(key, part):
    base = jnp.clip(jax.random.normal(jax.random.fold_in(key, 401), (TOKENS, D), jnp.float32), -6.0, 6.0)
    row_scale = jnp.exp(jax.random.uniform(jax.random.fold_in(key, 402), (TOKENS, 1), jnp.float32, jnp.log(0.3), jnp.log(3.0)))
    col_scale = jnp.exp(jax.random.uniform(jax.random.fold_in(key, 403), (1, D), jnp.float32, jnp.log(0.3), jnp.log(3.0)))
    return (base * row_scale * col_scale).astype(jnp.bfloat16)


def load_order(key):
    return jax.random.permutation(jax.random.fold_in(key, 500), EXPERTS).astype(jnp.int32)


def block_routes(key, block_index, order):
    block_key = jax.random.fold_in(jax.random.fold_in(key, 501), block_index)
    n_entry = EXPERTS * MOST
    entry = jnp.arange(n_entry, dtype=jnp.int32)
    ranked = entry // MOST
    copy_index = entry % MOST
    weight_copy = jnp.where(ranked >= EXPERTS // 2, 3, 1).astype(jnp.int32)
    noise = jax.random.randint(block_key, (n_entry,), 0, 65536, jnp.int32)
    score = noise + copy_index * 16384 * weight_copy
    n_blocks = TOKENS // REQ_DEV
    cold_pick = EXPERTS // 2 + block_index % (EXPERTS - EXPERTS // 2)
    forced = (ranked == 0) | (ranked == cold_pick) | (copy_index == 0) & (ranked % n_blocks == block_index)
    score = jnp.where(forced, -1, score).astype(jnp.int32)
    picked = jnp.argsort(score, stable=True)[:REQ_DEV * TOP].astype(jnp.int32)
    picked = jnp.sort(picked)
    grid = order[picked // MOST].reshape(TOP, REQ_DEV).T
    shuffle = jax.random.permutation(jax.random.fold_in(block_key, 7), REQ_DEV)
    return grid[shuffle].astype(jnp.int32)


def draw_expert_ids(key, part):
    order = load_order(key)
    n_blocks = TOKENS // REQ_DEV
    blocks = jax.vmap(lambda index: block_routes(key, index, order))(jnp.arange(n_blocks, dtype=jnp.int32))
    return blocks.reshape(TOKENS, TOP).astype(jnp.int32)


def replica_table(key):
    order = load_order(key)
    hottest = order[:EXPERTS // 2]
    table = jnp.concatenate([order, hottest, hottest])
    shuffle = jax.random.permutation(jax.random.fold_in(key, 204), SLOTS)
    return table[shuffle].astype(jnp.int32)


def draw_replica_map(key, part):
    return replica_table(key)


def draw_w_gate(key, part):
    base = (jax.random.normal(jax.random.fold_in(key, 301), (EXPERTS, D, HID), jnp.float32) * D ** (-0.5)).astype(jnp.bfloat16)
    return base[replica_table(key)]


def draw_w_up(key, part):
    base = (jax.random.normal(jax.random.fold_in(key, 302), (EXPERTS, D, HID), jnp.float32) * D ** (-0.5)).astype(jnp.bfloat16)
    return base[replica_table(key)]


def draw_w_down(key, part):
    base = (jax.random.normal(jax.random.fold_in(key, 303), (EXPERTS, HID, D), jnp.float32) * HID ** (-0.5)).astype(jnp.bfloat16)
    return base[replica_table(key)]


def with_ends(entries, stream_key, least, largest):
    longest = entries.shape.index(max(entries.shape))
    spots = []
    for shift in (0, 1):
        where = [jax.random.randint(jax.random.fold_in(stream_key, axis), (), 0, length) for axis, length in enumerate(entries.shape)]
        where[longest] = (where[longest] + shift) % entries.shape[longest]
        spots.append(tuple(where))
    return entries.at[spots[0]].set(least).at[spots[1]].set(largest)


def block_levels(key, dims, pieces, least, high):
    def one(axis_at, blocks):
        heights = jax.random.uniform(jax.random.fold_in(jax.random.fold_in(key, 6), axis_at), (blocks,), jnp.float32, least / len(pieces), high / len(pieces))
        return jnp.repeat(jnp.exp(heights), dims[axis_at] // blocks).reshape((-1,) + (1,) * (len(dims) - axis_at - 1))

    loudness = one(*pieces[0])
    for cut in pieces[1:]:
        loudness = loudness * one(*cut)
    return loudness


def bell_draw(rng, dims, width, most, cuts=(), kind=jnp.bfloat16):
    entries = width * jax.random.normal(rng, dims, jnp.float32)
    if cuts:
        entries = entries * block_levels(rng, dims, cuts, -0.22, 0.18)
    return jnp.clip(entries, -most, most).astype(kind)


def setup_inputs(seed: int = 0) -> dict:
    key_of = jax.random.split(jax.random.key(seed), 14)
    queries = draw_queries(jax.random.fold_in(key_of[13], 71), 0)
    keys = draw_keys(jax.random.fold_in(key_of[13], 71), 0)
    values = bell_draw(key_of[2], (TOKENS, KVH, CACHE, HD), 1.0, 6.0, ((0, 8), (1, 4)))
    lengths = with_ends(jax.random.randint(key_of[3], (TOKENS,), 2, CACHE + 1), jax.random.fold_in(key_of[3], 1), 2, CACHE).astype(jnp.int32)
    out_weight = bell_draw(key_of[4], (HEADS * HD, D), (HEADS * HD) ** -0.5, 0.125, ((0, 8),))
    residual = draw_residual(jax.random.fold_in(key_of[13], 71), 0)
    norm_gain = jnp.clip(jnp.exp(jax.random.uniform(key_of[6], (D,), jnp.float32, math.log(0.5), math.log(2.0))), 0.5, 2.0)
    expert_ids = draw_expert_ids(jax.random.fold_in(key_of[13], 71), 0)
    gate_weights = jnp.clip(jnp.exp(math.log(1.0) - 1.609438 * jax.random.uniform(key_of[8], (TOKENS, TOP), jnp.float32) ** block_levels(key_of[8], (TOKENS, TOP), ((0, 4),), -0.2, 0.2)), 0.2, 1.0)
    replica_map = draw_replica_map(jax.random.fold_in(key_of[13], 71), 0)
    w_gate = draw_w_gate(jax.random.fold_in(key_of[13], 71), 0)
    w_up = draw_w_up(jax.random.fold_in(key_of[13], 71), 0)
    w_down = draw_w_down(jax.random.fold_in(key_of[13], 71), 0)
    return dict(queries=queries, keys=keys, values=values, lengths=lengths, out_weight=out_weight, residual=residual, norm_gain=norm_gain, expert_ids=expert_ids, gate_weights=gate_weights, replica_map=replica_map, w_gate=w_gate, w_up=w_up, w_down=w_down)


def reference(queries, keys, values, lengths, out_weight, residual, norm_gain, expert_ids, gate_weights, replica_map, w_gate, w_up, w_down):
    f32 = jnp.float32
    n_tok = queries.shape[0]
    group = HEADS // KVH
    query = queries.astype(f32).reshape(n_tok, KVH, group, HD)
    scores = jnp.einsum('tgqd,tgpd->tgqp', query, keys.astype(f32), precision=lax.Precision.HIGHEST) * HD ** (-0.5)
    position = jnp.arange(CACHE, dtype=jnp.int32)
    valid = (position[None, :] < lengths[:, None])[:, None, None, :]
    scores = jnp.where(valid, scores, -1e+30)
    peak = lax.optimization_barrier(jnp.max(scores, axis=-1, keepdims=True))
    weights = jnp.where(valid, jnp.exp(scores - peak), 0.0)
    probs = weights / lax.optimization_barrier(jnp.sum(weights, axis=-1, keepdims=True))
    attended = jnp.einsum('tgqp,tgpd->tgqd', probs, values.astype(f32), precision=lax.Precision.HIGHEST)
    attended = attended.astype(jnp.bfloat16).reshape(n_tok, HEADS * HD)
    attn_out = jnp.dot(attended, out_weight, preferred_element_type=f32)
    mixed = residual.astype(f32) + attn_out
    scale = lax.rsqrt(lax.optimization_barrier(jnp.mean(mixed * mixed, axis=1)) + 1e-06)
    normed = (mixed * scale[:, None] * norm_gain[None, :]).astype(jnp.bfloat16)
    probs_top = gate_weights / lax.optimization_barrier(jnp.sum(gate_weights, axis=1, keepdims=True))
    flat_ids = expert_ids.reshape(-1)
    n_pairs = flat_ids.shape[0]
    flat_probs = jnp.concatenate([probs_top.reshape(-1), jnp.zeros((1,), f32)])
    flat_rows = jnp.concatenate([jnp.arange(n_pairs, dtype=jnp.int32) // TOP, jnp.full((1,), n_tok, jnp.int32)])
    padded = jnp.concatenate([normed, jnp.zeros((1, D), jnp.bfloat16)], axis=0)
    bound = MOST * N_REQ
    half = HID // 2

    def one_expert(moe, expert):
        chosen = jnp.nonzero(flat_ids == expert, size=bound, fill_value=n_pairs)[0].astype(jnp.int32)
        rows_idx = flat_rows[chosen]
        weight = flat_probs[chosen]
        slot = jnp.argmax(replica_map == expert).astype(jnp.int32)
        rows = padded[rows_idx]
        gate = jnp.dot(rows, w_gate[slot], preferred_element_type=f32)
        up = jnp.dot(rows, w_up[slot], preferred_element_type=f32)
        act = (jax.nn.silu(gate) * up).astype(jnp.bfloat16)
        down = w_down[slot]
        low = jnp.dot(act[:, :half], down[:half], preferred_element_type=f32).astype(jnp.bfloat16)
        high = jnp.dot(act[:, half:], down[half:], preferred_element_type=f32).astype(jnp.bfloat16)
        low = lax.optimization_barrier(low)
        high = lax.optimization_barrier(high)
        out = (low.astype(f32) + high.astype(f32)).astype(jnp.bfloat16)
        out = lax.optimization_barrier(out)
        moe = moe.at[rows_idx].add(out.astype(f32) * weight[:, None], mode='drop')
        return (moe, None)
    moe, _ = lax.scan(one_expert, jnp.zeros((n_tok, D), f32), jnp.arange(EXPERTS, dtype=jnp.int32))
    return (mixed + moe).astype(jnp.bfloat16)
```

```python
import jax
import jax.numpy as jnp
from jax import lax
from jax.experimental import pallas as pl
from jax.experimental.pallas import tpu as pltpu
from jax.sharding import PartitionSpec as P


def swapped(value, axis, apart):
    mask = 2**apart
    pairs = [(source, source ^ mask) for source in range(lax.axis_size(axis))]
    return lax.ppermute(value, axis, pairs)


def expert_runner(w_gate, w_up, w_down, complete, n_kvh, n_exp, block):

    def run(received):
        full = complete(received)
        lead_a = full.shape[0]
        lead_b = full.shape[1]
        d_model = w_gate.shape[1]
        rows = full.reshape(lead_a * lead_b, d_model)
        gate = jnp.dot(rows, w_gate[0], preferred_element_type=jnp.float32)
        up = jnp.dot(rows, w_up[0], preferred_element_type=jnp.float32)
        act = (jax.nn.silu(gate) * up).astype(jnp.bfloat16)
        down = jnp.dot(act, w_down[0], preferred_element_type=jnp.float32)
        terms = down.reshape(lead_a, lead_b, n_kvh, n_exp, block)
        summed = lax.psum_scatter(
            terms.astype(jnp.bfloat16), "exp", scatter_dimension=3, tiled=True
        )
        back = summed.reshape(lead_a, lead_b, n_kvh * block)
        return lax.all_to_all(back, "req", split_axis=0, concat_axis=0, tiled=True)

    return run


def routed_shards(
    queries,
    keys,
    values,
    lengths,
    out_weight,
    residual,
    norm_gain,
    expert_ids,
    gate_weights,
    replica_map,
    w_gate,
    w_up,
    w_down,
):
    f32 = jnp.float32
    half_rows_count = queries.shape[0]
    n_rows = lengths.shape[0]
    head_dim = keys.shape[3]
    span = keys.shape[2]
    heads_here = queries.shape[1] // head_dim
    n_kvh = lax.axis_size("kvh")
    n_exp = lax.axis_size("exp")
    n_req = lax.axis_size("req")
    side = lax.axis_index("exp")
    own_lengths = lax.dynamic_slice_in_dim(lengths, side * half_rows_count, half_rows_count, 0)
    query = queries.reshape(half_rows_count, heads_here, head_dim)
    scores = jnp.einsum(
        "rhd,rpd->rhp", query, keys[:, 0], preferred_element_type=f32
    ) * head_dim ** (-0.5)
    position = lax.broadcasted_iota(jnp.int32, (1, 1, span), 2)
    valid = position < own_lengths[:, None, None]
    scores = jnp.where(valid, scores, -1e30)
    peak = jnp.max(scores, axis=-1)
    weights = jnp.where(valid, jnp.exp(scores - peak[..., None]), 0.0)
    total = jnp.sum(weights, axis=-1)
    probs = weights / total[..., None]
    numer = jnp.einsum(
        "rhp,rpd->rhd", probs, values[:, 0].astype(f32), precision=lax.Precision.HIGHEST
    )
    attended_part = numer.astype(jnp.bfloat16).reshape(half_rows_count, heads_here * head_dim)
    attended = lax.all_gather(attended_part, "exp", axis=0, tiled=True)
    cut = out_weight.shape[0]
    own_heads = lax.dynamic_slice_in_dim(attended, side * cut, cut, 1)
    d_model = out_weight.shape[1]
    block = d_model // (n_kvh * n_exp)
    attn_block = (
        lax.psum_scatter(
            lax.dot_general(
                out_weight, own_heads, (((0,), (1,)), ((), ())), preferred_element_type=f32
            ).astype(jnp.bfloat16),
            ("kvh", "exp"),
            scatter_dimension=0,
            tiled=True,
        )
        .astype(jnp.float32)
        .T
    )
    offset = lax.axis_index(("kvh", "exp")) * block
    mixed = lax.dynamic_slice_in_dim(residual, offset, block, 1).astype(f32) + attn_block
    squares = lax.psum(jnp.sum(mixed * mixed, axis=1), ("kvh", "exp"))
    scale = lax.rsqrt(squares / d_model + 1e-06)
    gain_block = lax.dynamic_slice_in_dim(norm_gain, offset, block, 0)
    normed = (mixed * scale[:, None] * gain_block[None, :]).astype(jnp.bfloat16)
    top = expert_ids.shape[1]
    n_slots = replica_map.shape[0]
    n_experts = n_slots // 2
    capacity = min(n_rows, max(2, (3 * n_rows * top + 2 * n_experts - 1) // (2 * n_experts)))
    probs_top = gate_weights / jnp.sum(gate_weights, axis=1, keepdims=True)
    expert_range = jnp.arange(n_experts, dtype=jnp.int32)
    owned = (replica_map[:, None] == expert_range[None, :]).astype(jnp.int32)
    earlier = jnp.cumsum(owned, axis=0) - owned
    rank = jnp.sum(earlier * owned, axis=1)
    copies = jnp.sum(owned, axis=0)
    picked = (expert_ids[..., None] == expert_range).astype(jnp.int32)
    copies_pair = jnp.sum(picked * copies, axis=-1)
    turn = jnp.full((n_rows, top), lax.axis_index("req"), jnp.int32)
    which = turn % copies_pair
    match = (replica_map == expert_ids[..., None]) & (rank == which[..., None])
    slot = jnp.argmax(match, axis=-1)
    mine = slot % n_kvh == lax.axis_index("kvh")
    flat_dest = (slot // n_kvh).reshape(-1)
    flat_mine = mine.reshape(-1)
    toward = (
        (flat_dest[:, None] == jnp.arange(n_req, dtype=jnp.int32)[None, :]) & flat_mine[:, None]
    ).astype(jnp.int32)
    before = jnp.cumsum(toward, axis=0) - toward
    place = jnp.sum(before * toward, axis=1)
    n_buffer = n_req * capacity
    target = jnp.where(flat_mine, flat_dest * capacity + place, n_buffer)
    row_of = jnp.arange(n_rows * top, dtype=jnp.int32) // top
    source = jnp.full((n_buffer,), -1, jnp.int32).at[target].set(row_of, mode="drop")
    half_rows = lax.all_gather(normed.reshape(n_rows, 1, block), "kvh", axis=1, tiled=True).reshape(
        n_rows, n_kvh * block
    )

    def complete(received):
        partner = swapped(received, "exp", 0)
        lead_a = received.shape[0]
        lead_b = received.shape[1]
        own_part = received.reshape(lead_a, lead_b, n_kvh, 1, block)
        other_part = partner.reshape(lead_a, lead_b, n_kvh, 1, block)
        first = jnp.where(side == 0, own_part, other_part)
        second = jnp.where(side == 0, other_part, own_part)
        return jnp.concatenate([first, second], axis=3).reshape(lead_a, lead_b, n_kvh * 2 * block)

    runner = expert_runner(w_gate, w_up, w_down, complete, n_kvh, n_exp, block)
    taken = half_rows[jnp.maximum(source, 0)]
    returned = runner(
        lax.all_to_all(
            jnp.where(source[:, None] >= 0, taken, jnp.zeros((), jnp.bfloat16)).reshape(
                n_req, capacity, half_rows.shape[1]
            ),
            "req",
            split_axis=0,
            concat_axis=0,
            tiled=True,
        )
    )
    flat_back = returned.reshape(n_buffer, n_kvh * block)
    gathered = flat_back[jnp.minimum(target, n_buffer - 1)].reshape(n_rows, top, n_kvh * block)
    weight = jnp.where(mine, probs_top, 0.0)
    partial_value = jnp.zeros((n_rows, n_kvh * block), f32)
    for entry in range(top):
        partial_value = partial_value + weight[:, entry, None] * gathered[:, entry].astype(f32)
    moe_block = (
        lax.psum_scatter(
            partial_value.reshape(n_rows, n_kvh, block).astype(jnp.bfloat16),
            "kvh",
            scatter_dimension=1,
            tiled=True,
        )
        .astype(jnp.float32)
        .reshape(n_rows, block)
    )
    return (mixed + moe_block).astype(jnp.bfloat16)


F32 = jnp.float32
BF16 = jnp.bfloat16
AXES = ("req", "kvh", "exp")
STEP = 16


def is_dense(sizes, args):
    queries, keys, expert_ids, replica_map = args[0], args[1], args[7], args[9]
    n_req, n_kvh, n_exp = sizes
    top = expert_ids.shape[1]
    span = keys.shape[2]
    powers = all(size & (size - 1) == 0 for size in (*sizes, span, queries.shape[0]))
    return (
        powers
        and n_req >= 2
        and n_kvh >= 2
        and n_exp == 2
        and top == replica_map.shape[0] // 2
        and queries.shape[0] % (2 * STEP) == 0
    )


def moved(value, d_req, d_kvh, d_exp):
    n_req, n_kvh, n_exp = (lax.axis_size(axis) for axis in AXES)
    pairs = []
    for req in range(n_req):
        for kvh in range(n_kvh):
            for exp in range(n_exp):
                source = (req * n_kvh + kvh) * n_exp + exp
                target = ((req ^ d_req) * n_kvh + (kvh ^ d_kvh)) * n_exp + (exp ^ d_exp)
                pairs.append((source, target))
    return lax.ppermute(value, AXES, pairs)


def place():
    kvh = lax.axis_index("kvh")
    return lax.axis_index("req"), kvh // 2, kvh % 2, lax.axis_index("exp")


def nt_dot(left, right, **kwargs):
    return lax.dot_general(
        left, right, (((1,), (1,)), ((), ())), preferred_element_type=F32, **kwargs
    )


def nn_dot(left, right):
    return jnp.dot(left, right, preferred_element_type=F32)


def in_vmem(count):
    return [pl.BlockSpec(memory_space=pltpu.VMEM)] * count


def in_smem():
    return pl.BlockSpec(memory_space=pltpu.SMEM)


def called(kernel, args, outs, flops, n_smem=0, scratch=(), name=None):
    moves = sum(arg.size * arg.dtype.itemsize for arg in (*args, *outs))
    return pl.pallas_call(
        kernel,
        out_shape=tuple(outs),
        in_specs=[in_smem()] * n_smem + in_vmem(len(args) - n_smem),
        out_specs=tuple(in_vmem(len(outs))),
        scratch_shapes=list(scratch),
        cost_estimate=pl.CostEstimate(flops=flops, bytes_accessed=moves, transcendentals=0),
        name=name,
    )(*args)


def like(shape, dtype):
    return jax.ShapeDtypeStruct(shape, dtype)


def attention_kernel(lengths, query, key, value, ids, gates, *outs):
    blocks, shares = outs[:4], outs[4]
    step = pl.program_id(0)
    _, _, core, side = place()
    n = query.shape[0]
    span, head_dim = key.shape[2], key.shape[3]
    heads = query.shape[1] // head_dim
    steps = pl.num_programs(0)

    @pl.when(step == 0)
    def _():
        probs_top = gates[...] / jnp.sum(gates[...], axis=0, keepdims=True)
        for expert in range(shares.shape[0]):
            shares[expert : expert + 1, :] = jnp.sum(
                jnp.where(ids[...] == expert, probs_top, 0.0), axis=0, keepdims=True
            )

    rows = jnp.concatenate(
        [query[:, head * head_dim : (head + 1) * head_dim] for head in range(heads)], axis=0
    )
    scores = nt_dot(rows, key[...].reshape(n * span, head_dim)) * head_dim ** (-0.5)
    column = lax.broadcasted_iota(jnp.int32, (1, n * span), 1)
    owner = lax.shift_right_logical(column, span.bit_length() - 1)
    limit = jnp.zeros((1, n * span), jnp.int32)
    first = (side * steps + step) * n
    for index in range(n):
        limit = jnp.where(owner == index, lengths[first + index], limit)
    live = (column & (span - 1)) < limit
    request = lax.broadcasted_iota(jnp.int32, (heads * n, 1), 0) & (n - 1)
    valid = (request == owner) & live
    scores = jnp.where(valid, scores, -1e30)
    peak = jnp.max(scores, axis=1, keepdims=True)
    weights = jnp.where(valid, jnp.exp(scores - peak), 0.0)
    total = jnp.sum(weights, axis=1, keepdims=True)
    high = weights.astype(BF16)
    low = (weights - high.astype(F32)).astype(BF16)
    held = value[...].reshape(n * span, head_dim)
    numer = (nn_dot(high, held) + nn_dot(low, held)) / total
    by_head = [numer[head * n : (head + 1) * n].astype(BF16) for head in range(heads)]
    parts = heads // 2
    lower = jnp.concatenate(by_head[:parts], axis=1)
    upper = jnp.concatenate(by_head[parts:], axis=1)
    near = jnp.where(side == 0, lower, upper)
    far = jnp.where(side == 0, upper, lower)
    half = steps // 2
    target_core = step // half
    spot = pl.ds(pl.multiple_of((step % half) * n, n), n)

    @pl.when(target_core == core)
    def _():
        blocks[0][spot, :] = near
        blocks[1][spot, :] = far

    @pl.when(target_core != core)
    def _():
        blocks[2][spot, :] = near
        blocks[3][spot, :] = far


def attention(queries, keys, values, lengths, ids, gates, n_experts):
    rows = queries.shape[0]
    steps = rows // STEP
    span, head_dim = keys.shape[2], keys.shape[3]
    piece = like((rows // 2, queries.shape[1] // 2), BF16)
    outs = [piece] * 4 + [like((n_experts, ids.shape[1]), F32)]
    whole = lambda shape: pl.BlockSpec(shape, lambda step: (0, 0))
    cache = pl.BlockSpec((STEP, 1, span, head_dim), lambda step: (step, 0, 0, 0))
    return pl.pallas_call(
        attention_kernel,
        grid=(steps,),
        out_shape=tuple(outs),
        in_specs=[
            in_smem(),
            pl.BlockSpec((STEP, queries.shape[1]), lambda step: (step, 0)),
            cache,
            cache,
            whole(ids.shape),
            whole(gates.shape),
        ],
        out_specs=tuple(whole(out.shape) for out in outs),
        cost_estimate=pl.CostEstimate(
            flops=6 * STEP * rows * queries.shape[1] * span,
            bytes_accessed=2 * keys.size * 2,
            transcendentals=0,
        ),
        name="attention",
    )(lengths, queries, keys, values, ids, gates)


def columns_of(d_exp, d_row, index, block):
    _, row, _, side = place()
    return pl.multiple_of((((row ^ d_row) * 2 + index) * 2 + (side ^ d_exp)) * block, block)


def projection_kernel(chips, *refs):
    pieces, (near_weight, far_weight, residual), outs = refs[:4], refs[4:7], refs[7:-2]
    near, far = refs[-2:]
    _, _, core, side = place()
    rows = pieces[0].shape[0]
    block = outs[0].shape[1] // 2
    spots = [pl.ds(pl.multiple_of((side ^ d) * rows, rows), rows) for d in range(2)]
    for d in range(2):
        near[spots[d], :] = pieces[d][...]
        far[spots[d], :] = pieces[2 + d][...]
    for chip, (d_exp, d_row) in enumerate(chips):
        for index in range(2):
            start = columns_of(d_exp, d_row, index, block)
            where = pl.ds(start, block)
            part = nn_dot(near[...], near_weight[:, where]) + nn_dot(far[...], far_weight[:, where])
            here = slice(index * block, (index + 1) * block)
            if chip:
                outs[chip][:, here] = part.astype(BF16)
                continue
            for half in range(2):
                own = slice(half * rows, (half + 1) * rows)
                at = pl.ds(pl.multiple_of((half * 2 + core) * rows, rows), rows)
                outs[0][own, here] = part[own] + residual[at, where].astype(F32)


def mixed_kernel(count, *refs):
    own, others, gain, mixed, sent = refs[0], refs[1:count], refs[count], refs[-2], refs[-1]
    block = own.shape[1] // 2
    for index in range(2):
        here = slice(index * block, (index + 1) * block)
        total = own[:, here]
        for other in others:
            total = total + other[:, here].astype(F32)
        mixed[:, here] = total
        scale = gain[:, pl.ds(columns_of(0, 0, index, block), block)]
        sent[:, here] = (total * scale).astype(BF16)


def share_of(slots, slot, group):
    expert = slots[slot]
    copies = jnp.int32(0)
    rank = jnp.int32(0)
    for index in range(slots.shape[0]):
        same = (slots[index] == expert).astype(jnp.int32)
        copies = copies + same
        rank = rank + jnp.where(index < slot, same, 0)
    return expert, (lax.rem(group, copies) == rank).astype(F32)


def expert_kernel(chips, groups, *refs):
    slots, gain = refs[0], refs[1]
    weights = refs[2:6]
    shares = refs[6 : 6 + len(groups)]
    parts = refs[6 + len(groups) : -1]
    act_ref = refs[-1]
    req, row, core, side = place()
    rows, width = parts[0].shape
    block = width // 2
    hidden, d_model = weights[0].shape
    gates = None
    squares = None
    for chip, (d_exp, d_row) in enumerate(chips):
        for index in range(2):
            where = pl.ds(columns_of(d_exp, d_row, index, block), block)
            here = slice(index * block, (index + 1) * block)
            part = jnp.concatenate(
                [parts[group * len(chips) + chip][:, here] for group in range(len(groups))], axis=0
            )
            weight = jnp.concatenate([ref[:, where] for ref in weights], axis=0)
            product = nt_dot(part, weight)
            plain = part.astype(F32) / gain[:, where]
            square = jnp.sum(plain * plain, axis=1, keepdims=True)
            gates = product if gates is None else gates + product
            squares = square if squares is None else squares + square
    scale = lax.rsqrt(squares / d_model + 1e-06)
    gate = gates[:, : 2 * hidden] * scale
    up = gates[:, 2 * hidden :] * scale
    act = gate / (1.0 + jnp.exp(-gate)) * up
    n_tokens = shares[0].shape[1]
    n_experts = shares[0].shape[0]
    quarter = rows // 2
    local = lax.broadcasted_iota(jnp.int32, (rows, 1), 0)
    token = local + jnp.where(local >= quarter, quarter, 0) + core * quarter
    lane = lax.broadcasted_iota(jnp.int32, (rows, n_tokens), 1)
    chosen = (lane == token).astype(F32)
    expert_lane = lax.broadcasted_iota(jnp.int32, (rows, n_experts), 1)
    n_kvh = lax.axis_size("kvh")
    own_slot = req * n_kvh + row * 2 + core
    other_slot = req * n_kvh + row * 2 + (1 - core)
    factors = []
    for group, d_req in enumerate(groups):
        table = nt_dot(chosen, shares[group][...], precision=lax.Precision.HIGHEST)
        pair = []
        for slot in (own_slot, other_slot):
            expert, serves = share_of(slots, slot, req ^ d_req)
            share = jnp.sum(jnp.where(expert_lane == expert, table, 0.0), axis=1, keepdims=True)
            pair.append(share * serves)
        factors.append(pair)
    first = jnp.concatenate([pair[0] for pair in factors], axis=0)
    second = jnp.concatenate([pair[1] for pair in factors], axis=0)
    unit = lax.broadcasted_iota(jnp.int32, act.shape, 1)
    act_ref[...] = (act * jnp.where(unit < hidden, first, second)).astype(BF16)


def pieces_kernel(chips, weight, *outs):
    block = outs[0].shape[1] // 2
    for out, (d_exp, d_row) in zip(outs, chips, strict=True):
        for index in range(2):
            where = pl.ds(columns_of(d_exp, d_row, index, block), block)
            out[:, index * block : (index + 1) * block] = weight[:, where]


def combine_kernel(count, groups, *refs):
    acts, near, far = refs[:count], refs[count : 2 * count], refs[2 * count : 3 * count]
    rest = refs[3 * count :]
    mixed = None
    if groups[0] == 0:
        mixed, rest = rest[0], rest[1:]
    _, _, core, _ = place()
    rows = acts[0].shape[0] // len(groups)
    total = None
    for act, low, high in zip(acts, near, far, strict=True):
        product = nn_dot(act[...], jnp.concatenate([low[...], high[...]], axis=0))
        total = product if total is None else total + product
    block = total.shape[1] // 2
    for index, d_req in enumerate(groups):
        part = total[index * rows : (index + 1) * rows]
        if d_req == 0:
            part = part + mixed[...]
        own = jnp.where(core == 0, part[:, :block], part[:, block:])
        other = jnp.where(core == 0, part[:, block:], part[:, :block])
        rest[2 * index][...] = own.astype(rest[2 * index].dtype)
        rest[2 * index + 1][...] = other.astype(rest[2 * index + 1].dtype)


def final_kernel(count, *refs):
    own, other, out = refs[:count], refs[count : 2 * count], refs[-1]
    _, _, core, _ = place()
    rows = own[0].shape[0] // 2
    for terms, place_of in ((own, core), (other, 1 - core)):
        total = terms[0][...]
        for term in terms[1:]:
            total = total + term[...].astype(F32)
        for half in range(2):
            at = pl.ds(pl.multiple_of((half * 2 + place_of) * rows, rows), rows)
            out[at, :] = total[half * rows : (half + 1) * rows].astype(BF16)


def dense_shards(
    queries,
    keys,
    values,
    lengths,
    out_weight,
    residual,
    norm_gain,
    expert_ids,
    gate_weights,
    replica_map,
    w_gate,
    w_up,
    w_down,
):
    n_req, n_kvh, n_exp = (lax.axis_size(axis) for axis in AXES)
    d_model = out_weight.shape[1]
    block = d_model // (n_kvh * n_exp)
    rows = queries.shape[0]
    n_experts = expert_ids.shape[1]
    hidden = w_gate.shape[2]
    chips = [(d_exp, d_row) for d_row in range(n_kvh // 2) for d_exp in range(n_exp)]
    n_chips = len(chips)
    gain = norm_gain.reshape(1, d_model)

    out_weight_far = moved(out_weight, 0, 1, 0)
    *blocks, shares = attention(
        queries, keys, values, lengths, expert_ids.T, gate_weights.T, n_experts
    )
    blocks[1] = moved(blocks[1], 0, 0, 1)
    blocks[2] = moved(blocks[2], 0, 1, 0)
    blocks[3] = moved(blocks[3], 0, 1, 1)
    down = called(
        lambda *refs: pieces_kernel(chips, *refs),
        (w_down[0],),
        [like((hidden, 2 * block), BF16)] * n_chips,
        flops=0,
        name="pieces",
    )
    w_in = [w_gate[0].T, w_up[0].T]
    w_in = [w_in[0], moved(w_in[0], 0, 1, 0), w_in[1], moved(w_in[1], 0, 1, 0)]
    wide = (rows, 2 * block)
    sums = called(
        lambda *refs: projection_kernel(chips, *refs),
        (*blocks, out_weight, out_weight_far, residual),
        [like(wide, F32)] + [like(wide, BF16)] * (n_chips - 1),
        flops=4 * rows * out_weight.size,
        scratch=[pltpu.VMEM((rows, blocks[0].shape[1]), BF16)] * 2,
        name="projection",
    )
    sums = [
        sums[chip] if chip == 0 else moved(sums[chip], 0, 2 * d_row, d_exp)
        for chip, (d_exp, d_row) in enumerate(chips)
    ]
    down = [
        down[chip] if chip == 0 else moved(down[chip], 0, 2 * d_row, d_exp)
        for chip, (d_exp, d_row) in enumerate(chips)
    ]
    down_far = [moved(piece, 0, 1, 0) for piece in down]
    mixed, sent = called(
        lambda *refs: mixed_kernel(n_chips, *refs),
        (*sums, gain),
        [like(wide, F32), like(wide, BF16)],
        flops=8 * rows * block,
        name="mixed",
    )
    by_group = [sent if d_req == 0 else moved(sent, d_req, 0, 0) for d_req in range(n_req)]
    shares = [shares if d_req == 0 else moved(shares, d_req, 0, 0) for d_req in range(n_req)]
    half = n_req // 2
    near_terms, far_terms = [], []
    for groups in (range(half), range(half, n_req)):
        groups = tuple(groups)
        parts = [
            by_group[d_req] if not (d_exp or d_row) else moved(by_group[d_req], 0, 2 * d_row, d_exp)
            for d_req in groups
            for d_exp, d_row in chips
        ]
        (act,) = called(
            lambda *refs, groups=groups: expert_kernel(chips, groups, *refs),
            (replica_map, gain, *w_in, *(shares[d_req] for d_req in groups), *parts),
            [like((half * rows, 2 * hidden), BF16)],
            flops=8 * half * rows * d_model * hidden,
            n_smem=1,
            name="experts",
        )
        acts = [
            act if not (d_exp or d_row) else moved(act, 0, 2 * d_row, d_exp)
            for d_exp, d_row in chips
        ]
        tail = (mixed,) if groups[0] == 0 else ()
        terms = called(
            lambda *refs, groups=groups: combine_kernel(n_chips, groups, *refs),
            (*acts, *down, *down_far, *tail),
            [
                like((rows, block), F32 if d_req == 0 else BF16)
                for d_req in groups
                for _ in range(2)
            ],
            flops=8 * half * rows * hidden * n_chips * block,
            name="combine",
        )
        for index, d_req in enumerate(groups):
            near, far = terms[2 * index], terms[2 * index + 1]
            near_terms.append(near if d_req == 0 else moved(near, d_req, 0, 0))
            far_terms.append(moved(far, d_req, 1, 0))
    (out,) = called(
        lambda *refs: final_kernel(n_req, *refs),
        (*near_terms, *far_terms),
        [like((2 * rows, block), BF16)],
        flops=4 * n_req * rows * block,
        name="final",
    )
    return out


def solution(mesh):
    in_specs = (
        P(("req", "exp"), "kvh"),
        P(("req", "exp"), "kvh", None, None),
        P(("req", "exp"), "kvh", None, None),
        P("req"),
        P(("kvh", "exp"), None),
        P("req", None),
        P(),
        P("req", None),
        P("req", None),
        P(),
        P(("req", "kvh"), None, "exp"),
        P(("req", "kvh"), None, "exp"),
        P(("req", "kvh"), "exp", None),
    )
    out_specs = P("req", ("kvh", "exp"))
    sizes = tuple(mesh.shape[axis] for axis in ("req", "kvh", "exp"))

    def shards(*args):
        run = dense_shards if is_dense(sizes, args) else routed_shards
        return run(*args)

    return jax.shard_map(shards, mesh=mesh, in_specs=in_specs, out_specs=out_specs, check_vma=False)
```

```python
import jax
import jax.numpy as jnp
from jax import lax
from jax.experimental import pallas as pl
from jax.experimental.pallas import tpu as pltpu
from jax.sharding import PartitionSpec as P


def swapped(value, axis, apart):
    mask = 2**apart
    pairs = [(source, source ^ mask) for source in range(lax.axis_size(axis))]
    return lax.ppermute(value, axis, pairs)


def expert_runner(w_gate, w_up, w_down, complete, n_kvh, n_exp, block):

    def run(received):
        full = complete(received)
        lead_a = full.shape[0]
        lead_b = full.shape[1]
        d_model = w_gate.shape[1]
        rows = full.reshape(lead_a * lead_b, d_model)
        gate = jnp.dot(rows, w_gate[0], preferred_element_type=jnp.float32)
        up = jnp.dot(rows, w_up[0], preferred_element_type=jnp.float32)
        act = (jax.nn.silu(gate) * up).astype(jnp.bfloat16)
        down = jnp.dot(act, w_down[0], preferred_element_type=jnp.float32)
        terms = down.reshape(lead_a, lead_b, n_kvh, n_exp, block)
        summed = lax.psum_scatter(
            terms.astype(jnp.bfloat16), "exp", scatter_dimension=3, tiled=True
        )
        back = summed.reshape(lead_a, lead_b, n_kvh * block)
        return lax.all_to_all(back, "req", split_axis=0, concat_axis=0, tiled=True)

    return run


def routed_shards(
    queries,
    keys,
    values,
    lengths,
    out_weight,
    residual,
    norm_gain,
    expert_ids,
    gate_weights,
    replica_map,
    w_gate,
    w_up,
    w_down,
):
    f32 = jnp.float32
    half_rows_count = queries.shape[0]
    n_rows = lengths.shape[0]
    head_dim = keys.shape[3]
    span = keys.shape[2]
    heads_here = queries.shape[1] // head_dim
    n_kvh = lax.axis_size("kvh")
    n_exp = lax.axis_size("exp")
    n_req = lax.axis_size("req")
    side = lax.axis_index("exp")
    own_lengths = lax.dynamic_slice_in_dim(lengths, side * half_rows_count, half_rows_count, 0)
    query = queries.reshape(half_rows_count, heads_here, head_dim)
    scores = jnp.einsum(
        "rhd,rpd->rhp", query, keys[:, 0], preferred_element_type=f32
    ) * head_dim ** (-0.5)
    position = lax.broadcasted_iota(jnp.int32, (1, 1, span), 2)
    valid = position < own_lengths[:, None, None]
    scores = jnp.where(valid, scores, -1e30)
    peak = jnp.max(scores, axis=-1)
    weights = jnp.where(valid, jnp.exp(scores - peak[..., None]), 0.0)
    total = jnp.sum(weights, axis=-1)
    probs = weights / total[..., None]
    numer = jnp.einsum(
        "rhp,rpd->rhd", probs, values[:, 0].astype(f32), precision=lax.Precision.HIGHEST
    )
    attended_part = numer.astype(jnp.bfloat16).reshape(half_rows_count, heads_here * head_dim)
    attended = lax.all_gather(attended_part, "exp", axis=0, tiled=True)
    cut = out_weight.shape[0]
    own_heads = lax.dynamic_slice_in_dim(attended, side * cut, cut, 1)
    d_model = out_weight.shape[1]
    block = d_model // (n_kvh * n_exp)
    attn_block = (
        lax.psum_scatter(
            lax.dot_general(
                out_weight, own_heads, (((0,), (1,)), ((), ())), preferred_element_type=f32
            ).astype(jnp.bfloat16),
            ("kvh", "exp"),
            scatter_dimension=0,
            tiled=True,
        )
        .astype(jnp.float32)
        .T
    )
    offset = lax.axis_index(("kvh", "exp")) * block
    mixed = lax.dynamic_slice_in_dim(residual, offset, block, 1).astype(f32) + attn_block
    squares = lax.psum(jnp.sum(mixed * mixed, axis=1), ("kvh", "exp"))
    scale = lax.rsqrt(squares / d_model + 1e-06)
    gain_block = lax.dynamic_slice_in_dim(norm_gain, offset, block, 0)
    normed = (mixed * scale[:, None] * gain_block[None, :]).astype(jnp.bfloat16)
    top = expert_ids.shape[1]
    n_slots = replica_map.shape[0]
    n_experts = n_slots // 2
    capacity = min(n_rows, max(2, (3 * n_rows * top + 2 * n_experts - 1) // (2 * n_experts)))
    probs_top = gate_weights / jnp.sum(gate_weights, axis=1, keepdims=True)
    expert_range = jnp.arange(n_experts, dtype=jnp.int32)
    owned = (replica_map[:, None] == expert_range[None, :]).astype(jnp.int32)
    earlier = jnp.cumsum(owned, axis=0) - owned
    rank = jnp.sum(earlier * owned, axis=1)
    copies = jnp.sum(owned, axis=0)
    picked = (expert_ids[..., None] == expert_range).astype(jnp.int32)
    copies_pair = jnp.sum(picked * copies, axis=-1)
    turn = jnp.full((n_rows, top), lax.axis_index("req"), jnp.int32)
    which = turn % copies_pair
    match = (replica_map == expert_ids[..., None]) & (rank == which[..., None])
    slot = jnp.argmax(match, axis=-1)
    mine = slot % n_kvh == lax.axis_index("kvh")
    flat_dest = (slot // n_kvh).reshape(-1)
    flat_mine = mine.reshape(-1)
    toward = (
        (flat_dest[:, None] == jnp.arange(n_req, dtype=jnp.int32)[None, :]) & flat_mine[:, None]
    ).astype(jnp.int32)
    before = jnp.cumsum(toward, axis=0) - toward
    place = jnp.sum(before * toward, axis=1)
    n_buffer = n_req * capacity
    target = jnp.where(flat_mine, flat_dest * capacity + place, n_buffer)
    row_of = jnp.arange(n_rows * top, dtype=jnp.int32) // top
    source = jnp.full((n_buffer,), -1, jnp.int32).at[target].set(row_of, mode="drop")
    half_rows = lax.all_gather(normed.reshape(n_rows, 1, block), "kvh", axis=1, tiled=True).reshape(
        n_rows, n_kvh * block
    )

    def complete(received):
        partner = swapped(received, "exp", 0)
        lead_a = received.shape[0]
        lead_b = received.shape[1]
        own_part = received.reshape(lead_a, lead_b, n_kvh, 1, block)
        other_part = partner.reshape(lead_a, lead_b, n_kvh, 1, block)
        first = jnp.where(side == 0, own_part, other_part)
        second = jnp.where(side == 0, other_part, own_part)
        return jnp.concatenate([first, second], axis=3).reshape(lead_a, lead_b, n_kvh * 2 * block)

    runner = expert_runner(w_gate, w_up, w_down, complete, n_kvh, n_exp, block)
    taken = half_rows[jnp.maximum(source, 0)]
    returned = runner(
        lax.all_to_all(
            jnp.where(source[:, None] >= 0, taken, jnp.zeros((), jnp.bfloat16)).reshape(
                n_req, capacity, half_rows.shape[1]
            ),
            "req",
            split_axis=0,
            concat_axis=0,
            tiled=True,
        )
    )
    flat_back = returned.reshape(n_buffer, n_kvh * block)
    gathered = flat_back[jnp.minimum(target, n_buffer - 1)].reshape(n_rows, top, n_kvh * block)
    weight = jnp.where(mine, probs_top, 0.0)
    partial_value = jnp.zeros((n_rows, n_kvh * block), f32)
    for entry in range(top):
        partial_value = partial_value + weight[:, entry, None] * gathered[:, entry].astype(f32)
    moe_block = (
        lax.psum_scatter(
            partial_value.reshape(n_rows, n_kvh, block).astype(jnp.bfloat16),
            "kvh",
            scatter_dimension=1,
            tiled=True,
        )
        .astype(jnp.float32)
        .reshape(n_rows, block)
    )
    return (mixed + moe_block).astype(jnp.bfloat16)


F32 = jnp.float32
BF16 = jnp.bfloat16
AXES = ("req", "kvh", "exp")
STEP = 16
VMEM_LIMIT = 16 * 2**20


def is_dense(sizes, args):
    queries, keys, expert_ids, replica_map = args[0], args[1], args[7], args[9]
    n_req, n_kvh, n_exp = sizes
    top = expert_ids.shape[1]
    span = keys.shape[2]
    powers = all(size & (size - 1) == 0 for size in (*sizes, span, queries.shape[0]))
    return (
        powers
        and n_req >= 2
        and n_kvh >= 2
        and n_exp == 2
        and top == replica_map.shape[0] // 2
        and queries.shape[0] % (2 * STEP) == 0
    )


def moved(value, d_req, d_kvh, d_exp):
    n_req, n_kvh, n_exp = (lax.axis_size(axis) for axis in AXES)
    pairs = []
    for req in range(n_req):
        for kvh in range(n_kvh):
            for exp in range(n_exp):
                source = (req * n_kvh + kvh) * n_exp + exp
                target = ((req ^ d_req) * n_kvh + (kvh ^ d_kvh)) * n_exp + (exp ^ d_exp)
                pairs.append((source, target))
    return lax.ppermute(value, AXES, pairs)


def place():
    kvh = lax.axis_index("kvh")
    return lax.axis_index("req"), kvh // 2, kvh % 2, lax.axis_index("exp")


def nt_dot(left, right, **kwargs):
    return lax.dot_general(
        left, right, (((1,), (1,)), ((), ())), preferred_element_type=F32, **kwargs
    )


def nn_dot(left, right):
    return jnp.dot(left, right, preferred_element_type=F32)


def in_vmem(count):
    return [pl.BlockSpec(memory_space=pltpu.VMEM)] * count


def in_smem():
    return pl.BlockSpec(memory_space=pltpu.SMEM)


def called(kernel, args, outs, flops, n_smem=0, scratch=(), name=None):
    moves = sum(arg.size * arg.dtype.itemsize for arg in (*args, *outs))
    return pl.pallas_call(
        kernel,
        out_shape=tuple(outs),
        in_specs=[in_smem()] * n_smem + in_vmem(len(args) - n_smem),
        out_specs=tuple(in_vmem(len(outs))),
        scratch_shapes=list(scratch),
        compiler_params=pltpu.CompilerParams(vmem_limit_bytes=VMEM_LIMIT),
        cost_estimate=pl.CostEstimate(flops=flops, bytes_accessed=moves, transcendentals=0),
        name=name,
    )(*args)


def like(shape, dtype):
    return jax.ShapeDtypeStruct(shape, dtype)


def attention_kernel(lengths, query, key, value, ids, gates, *outs):
    blocks, shares = outs[:4], outs[4]
    step = pl.program_id(0)
    _, _, core, side = place()
    n = query.shape[0]
    span, head_dim = key.shape[2], key.shape[3]
    heads = query.shape[1] // head_dim
    steps = pl.num_programs(0)

    @pl.when(step == 0)
    def _():
        probs_top = gates[...] / jnp.sum(gates[...], axis=0, keepdims=True)
        for expert in range(shares.shape[0]):
            shares[expert : expert + 1, :] = jnp.sum(
                jnp.where(ids[...] == expert, probs_top, 0.0), axis=0, keepdims=True
            )

    rows = jnp.concatenate(
        [query[:, head * head_dim : (head + 1) * head_dim] for head in range(heads)], axis=0
    )
    scores = nt_dot(rows, key[...].reshape(n * span, head_dim)) * head_dim ** (-0.5)
    column = lax.broadcasted_iota(jnp.int32, (1, n * span), 1)
    owner = lax.shift_right_logical(column, span.bit_length() - 1)
    limit = jnp.zeros((1, n * span), jnp.int32)
    first = (side * steps + step) * n
    for index in range(n):
        limit = jnp.where(owner == index, lengths[first + index], limit)
    live = (column & (span - 1)) < limit
    request = lax.broadcasted_iota(jnp.int32, (heads * n, 1), 0) & (n - 1)
    valid = (request == owner) & live
    scores = jnp.where(valid, scores, -1e30)
    peak = jnp.max(scores, axis=1, keepdims=True)
    weights = jnp.where(valid, jnp.exp(scores - peak), 0.0)
    total = jnp.sum(weights, axis=1, keepdims=True)
    high = weights.astype(BF16)
    low = (weights - high.astype(F32)).astype(BF16)
    held = value[...].reshape(n * span, head_dim)
    numer = (nn_dot(high, held) + nn_dot(low, held)) / total
    by_head = [numer[head * n : (head + 1) * n].astype(BF16) for head in range(heads)]
    parts = heads // 2
    lower = jnp.concatenate(by_head[:parts], axis=1)
    upper = jnp.concatenate(by_head[parts:], axis=1)
    near = jnp.where(side == 0, lower, upper)
    far = jnp.where(side == 0, upper, lower)
    half = steps // 2
    target_core = step // half
    spot = pl.ds(pl.multiple_of((step % half) * n, n), n)

    @pl.when(target_core == core)
    def _():
        blocks[0][spot, :] = near
        blocks[1][spot, :] = far

    @pl.when(target_core != core)
    def _():
        blocks[2][spot, :] = near
        blocks[3][spot, :] = far


def attention(queries, keys, values, lengths, ids, gates, n_experts):
    rows = queries.shape[0]
    steps = rows // STEP
    span, head_dim = keys.shape[2], keys.shape[3]
    piece = like((rows // 2, queries.shape[1] // 2), BF16)
    outs = [piece] * 4 + [like((n_experts, ids.shape[1]), F32)]
    whole = lambda shape: pl.BlockSpec(shape, lambda step: (0, 0))
    cache = pl.BlockSpec((STEP, 1, span, head_dim), lambda step: (step, 0, 0, 0))
    return pl.pallas_call(
        attention_kernel,
        grid=(steps,),
        out_shape=tuple(outs),
        in_specs=[
            in_smem(),
            pl.BlockSpec((STEP, queries.shape[1]), lambda step: (step, 0)),
            cache,
            cache,
            whole(ids.shape),
            whole(gates.shape),
        ],
        out_specs=tuple(whole(out.shape) for out in outs),
        cost_estimate=pl.CostEstimate(
            flops=6 * STEP * rows * queries.shape[1] * span,
            bytes_accessed=2 * keys.size * 2,
            transcendentals=0,
        ),
        compiler_params=pltpu.CompilerParams(vmem_limit_bytes=VMEM_LIMIT),
        name="attention",
    )(lengths, queries, keys, values, ids, gates)


def columns_of(d_exp, d_row, index, block):
    _, row, _, side = place()
    return pl.multiple_of((((row ^ d_row) * 2 + index) * 2 + (side ^ d_exp)) * block, block)


def projection_kernel(chips, *refs):
    pieces, (near_weight, far_weight, residual), outs = refs[:4], refs[4:7], refs[7:-2]
    near, far = refs[-2:]
    _, _, core, side = place()
    rows = pieces[0].shape[0]
    block = outs[0].shape[1] // 2
    spots = [pl.ds(pl.multiple_of((side ^ d) * rows, rows), rows) for d in range(2)]
    for d in range(2):
        near[spots[d], :] = pieces[d][...]
        far[spots[d], :] = pieces[2 + d][...]
    for chip, (d_exp, d_row) in enumerate(chips):
        for index in range(2):
            start = columns_of(d_exp, d_row, index, block)
            where = pl.ds(start, block)
            part = nn_dot(near[...], near_weight[:, where]) + nn_dot(far[...], far_weight[:, where])
            here = slice(index * block, (index + 1) * block)
            if chip:
                outs[chip][:, here] = part.astype(BF16)
                continue
            for half in range(2):
                own = slice(half * rows, (half + 1) * rows)
                at = pl.ds(pl.multiple_of((half * 2 + core) * rows, rows), rows)
                outs[0][own, here] = part[own] + residual[at, where].astype(F32)


def own_tokens(rows, n_tokens, core):
    half = rows // 2
    local = lax.broadcasted_iota(jnp.int32, (rows, 1), 0)
    token = local + jnp.where(local >= half, half, 0) + core * half
    lane = lax.broadcasted_iota(jnp.int32, (rows, n_tokens), 1)
    return (lane == token).astype(F32)


def mixed_kernel(count, *refs):
    own, others, (gain, shares, mixed, sent) = refs[0], refs[1:count], refs[count:]
    rows = own.shape[0]
    block = own.shape[1] // 2
    _, _, core, _ = place()
    for index in range(2):
        here = slice(index * block, (index + 1) * block)
        total = own[:, here]
        for other in others:
            total = total + other[:, here].astype(F32)
        mixed[:, here] = total
        scale = gain[:, pl.ds(columns_of(0, 0, index, block), block)]
        sent[:rows, here] = (total * scale).astype(BF16)
    chosen = own_tokens(rows, shares.shape[1], core)
    table = nt_dot(shares[...], chosen, precision=lax.Precision.HIGHEST)
    high = table.astype(BF16)
    low = (table - high.astype(F32)).astype(BF16)
    rest = jnp.zeros((table.shape[0], 2 * block - 2 * rows), BF16)
    sent[rows:, :] = jnp.concatenate([high, low, rest], axis=1)


def joined_kernel(*refs):
    out = refs[-1]
    rows = out.shape[0] // (len(refs) - 1)
    for index, ref in enumerate(refs[:-1]):
        out[index * rows : (index + 1) * rows, :] = ref[:rows, :]


def share_of(slots, slot, group):
    expert = slots[slot]
    copies = jnp.int32(0)
    rank = jnp.int32(0)
    for index in range(slots.shape[0]):
        same = (slots[index] == expert).astype(jnp.int32)
        copies = copies + same
        rank = rank + jnp.where(index < slot, same, 0)
    return expert, (lax.rem(group, copies) == rank).astype(F32)


def expert_kernel(chips, groups, *refs):
    slots, gain = refs[0], refs[1]
    weights = refs[2:6]
    sents = refs[6 : 6 + len(groups)]
    parts = refs[6 + len(groups) : -1]
    act_ref = refs[-1]
    req, row, core, _ = place()
    rows = parts[0].shape[0] // len(groups)
    block = parts[0].shape[1] // 2
    hidden, d_model = weights[0].shape
    gates = None
    squares = None
    for part_ref, (d_exp, d_row) in zip(parts, chips, strict=True):
        for index in range(2):
            where = pl.ds(columns_of(d_exp, d_row, index, block), block)
            part = part_ref[:, index * block : (index + 1) * block]
            weight = jnp.concatenate([ref[:, where] for ref in weights], axis=0)
            product = nt_dot(part, weight)
            plain = part.astype(F32) / gain[:, where]
            square = jnp.sum(plain * plain, axis=1, keepdims=True)
            gates = product if gates is None else gates + product
            squares = square if squares is None else squares + square
    scale = lax.rsqrt(squares / d_model + 1e-06)
    gate = gates[:, : 2 * hidden] * scale
    up = gates[:, 2 * hidden :] * scale
    act = gate / (1.0 + jnp.exp(-gate)) * up
    n_experts = sents[0].shape[0] - rows
    lane = lax.broadcasted_iota(jnp.int32, (rows, 2 * rows), 1)
    local = lax.broadcasted_iota(jnp.int32, (rows, 2 * rows), 0)
    chosen = ((lane == local) | (lane == local + rows)).astype(BF16)
    expert_lane = lax.broadcasted_iota(jnp.int32, (rows, n_experts), 1)
    n_kvh = lax.axis_size("kvh")
    own_slot = req * n_kvh + row * 2 + core
    other_slot = req * n_kvh + row * 2 + (1 - core)
    factors = []
    for sent, d_req in zip(sents, groups, strict=True):
        table = nt_dot(chosen, sent[rows:, : 2 * rows])
        pair = []
        for slot in (own_slot, other_slot):
            expert, serves = share_of(slots, slot, req ^ d_req)
            share = jnp.sum(jnp.where(expert_lane == expert, table, 0.0), axis=1, keepdims=True)
            pair.append(share * serves)
        factors.append(pair)
    first = jnp.concatenate([pair[0] for pair in factors], axis=0)
    second = jnp.concatenate([pair[1] for pair in factors], axis=0)
    unit = lax.broadcasted_iota(jnp.int32, act.shape, 1)
    act_ref[...] = (act * jnp.where(unit < hidden, first, second)).astype(BF16)


def pieces_kernel(chips, weight, *outs):
    block = outs[0].shape[1] // 2
    for out, (d_exp, d_row) in zip(outs, chips, strict=True):
        for index in range(2):
            where = pl.ds(columns_of(d_exp, d_row, index, block), block)
            out[:, index * block : (index + 1) * block] = weight[:, where]


def combine_kernel(count, groups, *refs):
    acts, near, far = refs[:count], refs[count : 2 * count], refs[2 * count : 3 * count]
    rest = refs[3 * count :]
    mixed = None
    if 0 in groups:
        mixed, rest = rest[0], rest[1:]
    rows = acts[0].shape[0] // len(groups)
    total = None
    for act, low, high in zip(acts, near, far, strict=True):
        product = nn_dot(act[...], jnp.concatenate([low[...], high[...]], axis=0))
        total = product if total is None else total + product
    for index, (d_req, out) in enumerate(zip(groups, rest, strict=True)):
        part = total[index * rows : (index + 1) * rows]
        if d_req == 0:
            part = part + mixed[...]
        out[...] = part.astype(out.dtype)


def summed_kernel(*refs):
    terms, (own_out, other_out) = refs[:-2], refs[-2:]
    _, _, core, _ = place()
    total = terms[0][...]
    for term in terms[1:]:
        total = total + term[...].astype(F32)
    block = total.shape[1] // 2
    own_out[...] = jnp.where(core == 0, total[:, :block], total[:, block:]).astype(BF16)
    other_out[...] = jnp.where(core == 0, total[:, block:], total[:, :block]).astype(BF16)


def final_kernel(own, other, out):
    _, _, core, _ = place()
    rows = own.shape[0] // 2
    for part, place_of in ((own, core), (other, 1 - core)):
        for half in range(2):
            at = pl.ds(pl.multiple_of((half * 2 + place_of) * rows, rows), rows)
            out[at, :] = part[half * rows : (half + 1) * rows, :]


def exchanged(parts, chips):
    return [
        moved(part, 0, 2 * d_row, d_exp) if d_exp or d_row else part
        for part, (d_exp, d_row) in zip(parts, chips, strict=True)
    ]


def spread(value, chips):
    return exchanged([value] * len(chips), chips)


def dense_shards(
    queries,
    keys,
    values,
    lengths,
    out_weight,
    residual,
    norm_gain,
    expert_ids,
    gate_weights,
    replica_map,
    w_gate,
    w_up,
    w_down,
):
    n_req, n_kvh, n_exp = (lax.axis_size(axis) for axis in AXES)
    d_model = out_weight.shape[1]
    block = d_model // (n_kvh * n_exp)
    rows = queries.shape[0]
    n_experts = expert_ids.shape[1]
    hidden = w_gate.shape[2]
    chips = [(d_exp, d_row) for d_row in range(n_kvh // 2) for d_exp in range(n_exp)]
    n_chips = len(chips)
    gain = norm_gain.reshape(1, d_model)

    out_weight_far = moved(out_weight, 0, 1, 0)
    *blocks, shares = attention(
        queries, keys, values, lengths, expert_ids.T, gate_weights.T, n_experts
    )
    blocks[1] = moved(blocks[1], 0, 0, 1)
    blocks[2] = moved(blocks[2], 0, 1, 0)
    blocks[3] = moved(blocks[3], 0, 1, 1)
    down = called(
        lambda *refs: pieces_kernel(chips, *refs),
        (w_down[0],),
        [like((hidden, 2 * block), BF16)] * n_chips,
        flops=0,
        name="pieces",
    )
    w_in = [w_gate[0].T, w_up[0].T]
    w_in = [w_in[0], moved(w_in[0], 0, 1, 0), w_in[1], moved(w_in[1], 0, 1, 0)]
    wide = (rows, 2 * block)
    sums = called(
        lambda *refs: projection_kernel(chips, *refs),
        (*blocks, out_weight, out_weight_far, residual),
        [like(wide, F32)] + [like(wide, BF16)] * (n_chips - 1),
        flops=4 * rows * out_weight.size,
        scratch=[pltpu.VMEM((rows, blocks[0].shape[1]), BF16)] * 2,
        name="projection",
    )
    sums = exchanged(sums, chips)
    down = exchanged(down, chips)
    down_far = [moved(piece, 0, 1, 0) for piece in down]
    mixed, sent = called(
        lambda *refs: mixed_kernel(n_chips, *refs),
        (*sums, gain, shares),
        [like(wide, F32), like((rows + n_experts, 2 * block), BF16)],
        flops=8 * rows * block,
        name="mixed",
    )
    last = n_req - 1
    order = [last, *range(1, last)]
    by_group = {0: sent, **{d_req: moved(sent, d_req, 0, 0) for d_req in order}}
    half = n_req // 2
    order = [0, *order]
    terms = {}
    for groups in (tuple(order[:half]), tuple(order[half:])):
        (joined,) = called(
            joined_kernel,
            [by_group[d_req] for d_req in groups],
            [like((half * rows, 2 * block), BF16)],
            flops=0,
            name="joined",
        )
        parts = spread(joined, chips)
        (act,) = called(
            lambda *refs, groups=groups: expert_kernel(chips, groups, *refs),
            (replica_map, gain, *w_in, *(by_group[d_req] for d_req in groups), *parts),
            [like((half * rows, 2 * hidden), BF16)],
            flops=8 * half * rows * d_model * hidden,
            n_smem=1,
            name="experts",
        )
        tail = (mixed,) if 0 in groups else ()
        results = called(
            lambda *refs, groups=groups: combine_kernel(n_chips, groups, *refs),
            (*spread(act, chips), *down, *down_far, *tail),
            [like(wide, F32 if d_req == 0 else BF16) for d_req in groups],
            flops=8 * half * rows * hidden * n_chips * block,
            name="combine",
        )
        for d_req, result in zip(groups, results, strict=True):
            terms[d_req] = moved(result, d_req, 0, 0) if d_req else result
    own, other = called(
        summed_kernel,
        [terms[d_req] for d_req in order],
        [like((rows, block), BF16)] * 2,
        flops=4 * n_req * rows * block,
        name="summed",
    )
    (out,) = called(
        final_kernel,
        (own, moved(other, 0, 1, 0)),
        [like((2 * rows, block), BF16)],
        flops=4 * rows * block,
        name="final",
    )
    return out


def solution(mesh):
    in_specs = (
        P(("req", "exp"), "kvh"),
        P(("req", "exp"), "kvh", None, None),
        P(("req", "exp"), "kvh", None, None),
        P("req"),
        P(("kvh", "exp"), None),
        P("req", None),
        P(),
        P("req", None),
        P("req", None),
        P(),
        P(("req", "kvh"), None, "exp"),
        P(("req", "kvh"), None, "exp"),
        P(("req", "kvh"), "exp", None),
    )
    out_specs = P("req", ("kvh", "exp"))
    sizes = tuple(mesh.shape[axis] for axis in ("req", "kvh", "exp"))

    def shards(*args):
        run = dense_shards if is_dense(sizes, args) else routed_shards
        return run(*args)

    return jax.shard_map(shards, mesh=mesh, in_specs=in_specs, out_specs=out_specs, check_vma=False)
```

```python
import jax
import jax.numpy as jnp
from jax import lax
from jax.experimental import pallas as pl
from jax.experimental.pallas import tpu as pltpu
from jax.sharding import PartitionSpec as P


def swapped(value, axis, apart):
    mask = 2**apart
    pairs = [(source, source ^ mask) for source in range(lax.axis_size(axis))]
    return lax.ppermute(value, axis, pairs)


def expert_runner(w_gate, w_up, w_down, complete, n_kvh, n_exp, block):

    def run(received):
        full = complete(received)
        lead_a = full.shape[0]
        lead_b = full.shape[1]
        d_model = w_gate.shape[1]
        rows = full.reshape(lead_a * lead_b, d_model)
        gate = jnp.dot(rows, w_gate[0], preferred_element_type=jnp.float32)
        up = jnp.dot(rows, w_up[0], preferred_element_type=jnp.float32)
        act = (jax.nn.silu(gate) * up).astype(jnp.bfloat16)
        down = jnp.dot(act, w_down[0], preferred_element_type=jnp.float32)
        terms = down.reshape(lead_a, lead_b, n_kvh, n_exp, block)
        summed = lax.psum_scatter(
            terms.astype(jnp.bfloat16), "exp", scatter_dimension=3, tiled=True
        )
        back = summed.reshape(lead_a, lead_b, n_kvh * block)
        return lax.all_to_all(back, "req", split_axis=0, concat_axis=0, tiled=True)

    return run


def routed_shards(
    queries,
    keys,
    values,
    lengths,
    out_weight,
    residual,
    norm_gain,
    expert_ids,
    gate_weights,
    replica_map,
    w_gate,
    w_up,
    w_down,
):
    f32 = jnp.float32
    half_rows_count = queries.shape[0]
    n_rows = lengths.shape[0]
    head_dim = keys.shape[3]
    span = keys.shape[2]
    heads_here = queries.shape[1] // head_dim
    n_kvh = lax.axis_size("kvh")
    n_exp = lax.axis_size("exp")
    n_req = lax.axis_size("req")
    side = lax.axis_index("exp")
    own_lengths = lax.dynamic_slice_in_dim(lengths, side * half_rows_count, half_rows_count, 0)
    query = queries.reshape(half_rows_count, heads_here, head_dim)
    scores = jnp.einsum(
        "rhd,rpd->rhp", query, keys[:, 0], preferred_element_type=f32
    ) * head_dim ** (-0.5)
    position = lax.broadcasted_iota(jnp.int32, (1, 1, span), 2)
    valid = position < own_lengths[:, None, None]
    scores = jnp.where(valid, scores, -1e30)
    peak = jnp.max(scores, axis=-1)
    weights = jnp.where(valid, jnp.exp(scores - peak[..., None]), 0.0)
    total = jnp.sum(weights, axis=-1)
    probs = weights / total[..., None]
    numer = jnp.einsum(
        "rhp,rpd->rhd", probs, values[:, 0].astype(f32), precision=lax.Precision.HIGHEST
    )
    attended_part = numer.astype(jnp.bfloat16).reshape(half_rows_count, heads_here * head_dim)
    attended = lax.all_gather(attended_part, "exp", axis=0, tiled=True)
    cut = out_weight.shape[0]
    own_heads = lax.dynamic_slice_in_dim(attended, side * cut, cut, 1)
    d_model = out_weight.shape[1]
    block = d_model // (n_kvh * n_exp)
    attn_block = (
        lax.psum_scatter(
            lax.dot_general(
                out_weight, own_heads, (((0,), (1,)), ((), ())), preferred_element_type=f32
            ).astype(jnp.bfloat16),
            ("kvh", "exp"),
            scatter_dimension=0,
            tiled=True,
        )
        .astype(jnp.float32)
        .T
    )
    offset = lax.axis_index(("kvh", "exp")) * block
    mixed = lax.dynamic_slice_in_dim(residual, offset, block, 1).astype(f32) + attn_block
    squares = lax.psum(jnp.sum(mixed * mixed, axis=1), ("kvh", "exp"))
    scale = lax.rsqrt(squares / d_model + 1e-06)
    gain_block = lax.dynamic_slice_in_dim(norm_gain, offset, block, 0)
    normed = (mixed * scale[:, None] * gain_block[None, :]).astype(jnp.bfloat16)
    top = expert_ids.shape[1]
    n_slots = replica_map.shape[0]
    n_experts = n_slots // 2
    capacity = min(n_rows, max(2, (3 * n_rows * top + 2 * n_experts - 1) // (2 * n_experts)))
    probs_top = gate_weights / jnp.sum(gate_weights, axis=1, keepdims=True)
    expert_range = jnp.arange(n_experts, dtype=jnp.int32)
    owned = (replica_map[:, None] == expert_range[None, :]).astype(jnp.int32)
    earlier = jnp.cumsum(owned, axis=0) - owned
    rank = jnp.sum(earlier * owned, axis=1)
    copies = jnp.sum(owned, axis=0)
    picked = (expert_ids[..., None] == expert_range).astype(jnp.int32)
    copies_pair = jnp.sum(picked * copies, axis=-1)
    turn = jnp.full((n_rows, top), lax.axis_index("req"), jnp.int32)
    which = turn % copies_pair
    match = (replica_map == expert_ids[..., None]) & (rank == which[..., None])
    slot = jnp.argmax(match, axis=-1)
    mine = slot % n_kvh == lax.axis_index("kvh")
    flat_dest = (slot // n_kvh).reshape(-1)
    flat_mine = mine.reshape(-1)
    toward = (
        (flat_dest[:, None] == jnp.arange(n_req, dtype=jnp.int32)[None, :]) & flat_mine[:, None]
    ).astype(jnp.int32)
    before = jnp.cumsum(toward, axis=0) - toward
    place = jnp.sum(before * toward, axis=1)
    n_buffer = n_req * capacity
    target = jnp.where(flat_mine, flat_dest * capacity + place, n_buffer)
    row_of = jnp.arange(n_rows * top, dtype=jnp.int32) // top
    source = jnp.full((n_buffer,), -1, jnp.int32).at[target].set(row_of, mode="drop")
    half_rows = lax.all_gather(normed.reshape(n_rows, 1, block), "kvh", axis=1, tiled=True).reshape(
        n_rows, n_kvh * block
    )

    def complete(received):
        partner = swapped(received, "exp", 0)
        lead_a = received.shape[0]
        lead_b = received.shape[1]
        own_part = received.reshape(lead_a, lead_b, n_kvh, 1, block)
        other_part = partner.reshape(lead_a, lead_b, n_kvh, 1, block)
        first = jnp.where(side == 0, own_part, other_part)
        second = jnp.where(side == 0, other_part, own_part)
        return jnp.concatenate([first, second], axis=3).reshape(lead_a, lead_b, n_kvh * 2 * block)

    runner = expert_runner(w_gate, w_up, w_down, complete, n_kvh, n_exp, block)
    taken = half_rows[jnp.maximum(source, 0)]
    returned = runner(
        lax.all_to_all(
            jnp.where(source[:, None] >= 0, taken, jnp.zeros((), jnp.bfloat16)).reshape(
                n_req, capacity, half_rows.shape[1]
            ),
            "req",
            split_axis=0,
            concat_axis=0,
            tiled=True,
        )
    )
    flat_back = returned.reshape(n_buffer, n_kvh * block)
    gathered = flat_back[jnp.minimum(target, n_buffer - 1)].reshape(n_rows, top, n_kvh * block)
    weight = jnp.where(mine, probs_top, 0.0)
    partial_value = jnp.zeros((n_rows, n_kvh * block), f32)
    for entry in range(top):
        partial_value = partial_value + weight[:, entry, None] * gathered[:, entry].astype(f32)
    moe_block = (
        lax.psum_scatter(
            partial_value.reshape(n_rows, n_kvh, block).astype(jnp.bfloat16),
            "kvh",
            scatter_dimension=1,
            tiled=True,
        )
        .astype(jnp.float32)
        .reshape(n_rows, block)
    )
    return (mixed + moe_block).astype(jnp.bfloat16)


F32 = jnp.float32
BF16 = jnp.bfloat16
AXES = ("req", "kvh", "exp")
STEP = 16
VMEM_LIMIT = 16 * 2**20


def is_dense(sizes, args):
    queries, keys, expert_ids, replica_map = args[0], args[1], args[7], args[9]
    n_req, n_kvh, n_exp = sizes
    span = keys.shape[2]
    rows = queries.shape[0] // (n_req * n_exp)
    powers = all(size & (size - 1) == 0 for size in (*sizes, span, rows))
    fits = n_req >= 2 and n_kvh >= 2 and n_exp == 2 and rows % (2 * STEP) == 0
    return powers and fits and expert_ids.shape[1] == replica_map.shape[0] // 2


def moved(value, d_req, d_kvh, d_exp):
    n_req, n_kvh, n_exp = (lax.axis_size(axis) for axis in AXES)
    pairs = []
    for req in range(n_req):
        for kvh in range(n_kvh):
            for exp in range(n_exp):
                source = (req * n_kvh + kvh) * n_exp + exp
                target = ((req ^ d_req) * n_kvh + (kvh ^ d_kvh)) * n_exp + (exp ^ d_exp)
                pairs.append((source, target))
    return lax.ppermute(value, AXES, pairs)


def place():
    kvh = lax.axis_index("kvh")
    return lax.axis_index("req"), kvh // 2, kvh % 2, lax.axis_index("exp")


def nt_dot(left, right, **kwargs):
    return lax.dot_general(
        left, right, (((1,), (1,)), ((), ())), preferred_element_type=F32, **kwargs
    )


def nn_dot(left, right):
    return jnp.dot(left, right, preferred_element_type=F32)


def in_vmem(count):
    return [pl.BlockSpec(memory_space=pltpu.VMEM)] * count


def in_smem():
    return pl.BlockSpec(memory_space=pltpu.SMEM)


def called(kernel, args, outs, flops, n_smem=0, scratch=()):
    moves = sum(arg.size * arg.dtype.itemsize for arg in (*args, *outs))
    return pl.pallas_call(
        kernel,
        out_shape=tuple(outs),
        in_specs=[in_smem()] * n_smem + in_vmem(len(args) - n_smem),
        out_specs=tuple(in_vmem(len(outs))),
        scratch_shapes=list(scratch),
        compiler_params=pltpu.CompilerParams(vmem_limit_bytes=VMEM_LIMIT),
        cost_estimate=pl.CostEstimate(flops=flops, bytes_accessed=moves, transcendentals=0),
    )(*args)


def like(shape, dtype):
    return jax.ShapeDtypeStruct(shape, dtype)


def attention_kernel(chips, lengths, query, key, value, weight, down, *refs):
    blocks, weight_copy, pieces = refs[:4], refs[4], refs[5:-5]
    limits, rows_ref, key_ref, value_ref, sems = refs[-5:]
    _, _, core, side = place()
    n_rows = query.shape[0]
    span, head_dim = key.shape[2], key.shape[3]
    heads = query.shape[1] // head_dim
    n = STEP
    steps = n_rows // n
    half = steps // 2

    def cached(step, index):
        source, target = ((key, key_ref), (value, value_ref))[index]
        here = pl.ds(step * n, n)
        return pltpu.make_async_copy(source.at[here], target.at[here], sems.at[2 * step + index])

    begin = [
        pltpu.make_async_copy(query, rows_ref, sems.at[2 * steps]),
        pltpu.make_async_copy(lengths, limits, sems.at[2 * steps + 1]),
    ]
    rest = [pltpu.make_async_copy(weight, weight_copy, sems.at[2 * steps + 2])]
    block = pieces[0].shape[1] // 2
    for piece, (d_exp, d_row) in zip(pieces, chips, strict=True):
        for index in range(2):
            source = down.at[0, :, pl.ds(columns_of(d_exp, d_row, index, block), block)]
            target = piece.at[:, index * block : (index + 1) * block]
            sem = sems.at[2 * steps + 2 + len(rest)]
            rest.append(pltpu.make_async_copy(source, target, sem))
    for copy in begin:
        copy.start()
    for step in range(steps):
        for index in range(2):
            cached(step, index).start()
    for copy in rest:
        copy.start()
    column = lax.broadcasted_iota(jnp.int32, (1, n * span), 1)
    owner = lax.shift_right_logical(column, span.bit_length() - 1)
    position = column & (span - 1)
    request = lax.broadcasted_iota(jnp.int32, (heads * n, 1), 0) & (n - 1)
    same = request == owner
    for copy in begin:
        copy.wait()

    @pl.loop(0, steps)
    def _(step):
        here = pl.ds(pl.multiple_of(step * n, n), n)
        rows = jnp.concatenate(
            [rows_ref[here, head * head_dim : (head + 1) * head_dim] for head in range(heads)],
            axis=0,
        )
        limit = jnp.zeros((1, n * span), jnp.int32)
        first = side * n_rows + step * n
        for index in range(n):
            limit = jnp.where(owner == index, limits[first + index], limit)
        valid = same & (position < limit)
        cached(step, 0).wait()
        scores = nt_dot(rows, key_ref[here].reshape(n * span, head_dim)) * head_dim ** (-0.5)
        scores = jnp.where(valid, scores, -1e30)
        peak = jnp.max(scores, axis=1, keepdims=True)
        weights = jnp.exp(scores - peak)
        total = jnp.sum(weights, axis=1, keepdims=True)
        high = weights.astype(BF16)
        low = (weights - high.astype(F32)).astype(BF16)
        cached(step, 1).wait()
        held = value_ref[here].reshape(n * span, head_dim)
        both = nn_dot(jnp.concatenate([high, low], axis=0), held)
        numer = (both[: heads * n] + both[heads * n :]) / total
        by_head = [numer[head * n : (head + 1) * n].astype(BF16) for head in range(heads)]
        lower = jnp.concatenate(by_head[: heads // 2], axis=1)
        upper = jnp.concatenate(by_head[heads // 2 :], axis=1)
        near = jnp.where(side == 0, lower, upper)
        far = jnp.where(side == 0, upper, lower)
        passed = step >= half
        spot = pl.ds(pl.multiple_of((step - jnp.where(passed, half, 0)) * n, n), n)
        at_home = passed == (core == 1)

        @pl.when(at_home)
        def _():
            blocks[0][spot, :] = near
            blocks[1][spot, :] = far

        @pl.when(jnp.logical_not(at_home))
        def _():
            blocks[2][spot, :] = near
            blocks[3][spot, :] = far

    for copy in rest:
        copy.wait()


def attention(chips, queries, keys, values, lengths, out_weight, w_down, block):
    rows = queries.shape[0]
    span = keys.shape[2]
    piece = like((rows // 2, queries.shape[1] // 2), BF16)
    args = (lengths, queries, keys, values, out_weight, w_down)
    outs = [piece] * 4 + [like(out_weight.shape, BF16)]
    outs += [like((w_down.shape[1], 2 * block), BF16)] * len(chips)
    return pl.pallas_call(
        lambda *refs: attention_kernel(chips, *refs),
        out_shape=tuple(outs),
        in_specs=[pl.BlockSpec(memory_space=pltpu.HBM)] * len(args),
        out_specs=tuple(in_vmem(len(outs))),
        scratch_shapes=[
            pltpu.SMEM(lengths.shape, jnp.int32),
            pltpu.VMEM(queries.shape, BF16),
            pltpu.VMEM(keys.shape, BF16),
            pltpu.VMEM(values.shape, BF16),
            pltpu.SemaphoreType.DMA((3 + 2 * (rows // STEP) + 2 * len(chips),)),
        ],
        cost_estimate=pl.CostEstimate(
            flops=6 * STEP * rows * queries.shape[1] * span,
            bytes_accessed=2 * keys.size * 2,
            transcendentals=0,
        ),
        compiler_params=pltpu.CompilerParams(vmem_limit_bytes=VMEM_LIMIT),
        name="attention",
    )(*(pltpu.with_memory_space_constraint(arg, pltpu.HBM) for arg in args))


def routes_kernel(slots, ids, gates, shares, serves):
    probs_top = gates[...] / jnp.sum(gates[...], axis=0, keepdims=True)
    n_experts = shares.shape[0]
    for expert in range(n_experts):
        shares[expert : expert + 1, :] = jnp.sum(
            jnp.where(ids[...] == expert, probs_top, 0.0), axis=0, keepdims=True
        )
    req, row, core, _ = place()
    n_kvh = lax.axis_size("kvh")
    lane = lax.broadcasted_iota(jnp.int32, (1, n_experts), 1)
    n_req = serves.shape[0] // 2
    for index, at in enumerate((core, 1 - core)):
        slot = req * n_kvh + row * 2 + at
        expert = slots[slot]
        copies = jnp.int32(0)
        rank = jnp.int32(0)
        for other in range(slots.shape[0]):
            same = (slots[other] == expert).astype(jnp.int32)
            copies = copies + same
            rank = rank + jnp.where(other < slot, same, 0)
        for d_req in range(n_req):
            chosen = jnp.where(lax.rem(req ^ d_req, copies) == rank, expert, -1)
            serves[2 * d_req + index : 2 * d_req + index + 1, :] = (lane == chosen).astype(F32)


def columns_of(d_exp, d_row, index, block):
    _, row, _, side = place()
    return pl.multiple_of((((row ^ d_row) * 2 + index) * 2 + (side ^ d_exp)) * block, block)


def projection_kernel(chips, *refs):
    pieces, (near_weight, far_weight, residual), outs = refs[:4], refs[4:7], refs[7:-2]
    near, far = refs[-2:]
    _, _, core, side = place()
    rows = pieces[0].shape[0]
    block = outs[0].shape[1] // 2
    spots = [pl.ds(pl.multiple_of((side ^ d) * rows, rows), rows) for d in range(2)]
    for d in range(2):
        near[spots[d], :] = pieces[d][...]
        far[spots[d], :] = pieces[2 + d][...]
    for chip, (d_exp, d_row) in enumerate(chips):
        for index in range(2):
            start = columns_of(d_exp, d_row, index, block)
            where = pl.ds(start, block)
            part = nn_dot(near[...], near_weight[:, where]) + nn_dot(far[...], far_weight[:, where])
            here = slice(index * block, (index + 1) * block)
            if chip:
                outs[chip][:, here] = part.astype(BF16)
                continue
            for half in range(2):
                own = slice(half * rows, (half + 1) * rows)
                at = pl.ds(pl.multiple_of((half * 2 + core) * rows, rows), rows)
                outs[0][own, here] = part[own] + residual[at, where].astype(F32)


def own_tokens(rows, n_tokens, core):
    half = rows // 2
    local = lax.broadcasted_iota(jnp.int32, (rows, 1), 0)
    token = local + jnp.where(local >= half, half, 0) + core * half
    lane = lax.broadcasted_iota(jnp.int32, (rows, n_tokens), 1)
    return (lane == token).astype(F32)


def mixed_kernel(count, *refs):
    own, others, (gain, shares, mixed, sent) = refs[0], refs[1:count], refs[count:]
    rows = own.shape[0]
    block = own.shape[1] // 2
    _, _, core, _ = place()
    for index in range(2):
        here = slice(index * block, (index + 1) * block)
        total = own[:, here]
        for other in others:
            total = total + other[:, here].astype(F32)
        mixed[:, here] = total
        scale = gain[:, pl.ds(columns_of(0, 0, index, block), block)]
        sent[:rows, here] = (total * scale).astype(BF16)
    chosen = own_tokens(rows, shares.shape[1], core)
    table = nt_dot(shares[...], chosen, precision=lax.Precision.HIGHEST)
    high = table.astype(BF16)
    low = (table - high.astype(F32)).astype(BF16)
    rest = jnp.zeros((table.shape[0], 2 * block - 2 * rows), BF16)
    sent[rows:, :] = jnp.concatenate([high, low, rest], axis=1)


def joined_kernel(*refs):
    out = refs[-1]
    rows = out.shape[0] // (len(refs) - 1)
    for index, ref in enumerate(refs[:-1]):
        out[index * rows : (index + 1) * rows, :] = ref[:rows, :]


def expert_kernel(chips, groups, *refs):
    serves, gain = refs[0], refs[1]
    weights = refs[2:6]
    sents = refs[6 : 6 + len(groups)]
    parts = refs[6 + len(groups) : -1]
    act_ref = refs[-1]
    rows = parts[0].shape[0] // len(groups)
    block = parts[0].shape[1] // 2
    hidden, d_model = weights[0].shape
    gates = None
    squares = None
    for part_ref, (d_exp, d_row) in zip(parts, chips, strict=True):
        for index in range(2):
            where = pl.ds(columns_of(d_exp, d_row, index, block), block)
            part = part_ref[:, index * block : (index + 1) * block]
            weight = jnp.concatenate([ref[:, where] for ref in weights], axis=0)
            product = nt_dot(part, weight)
            plain = part.astype(F32) / gain[:, where]
            square = jnp.sum(plain * plain, axis=1, keepdims=True)
            gates = product if gates is None else gates + product
            squares = square if squares is None else squares + square
    scale = lax.rsqrt(squares / d_model + 1e-06)
    gate = gates[:, : 2 * hidden] * scale
    up = gates[:, 2 * hidden :] * scale
    act = gate / (1.0 + jnp.exp(-gate)) * up
    lane = lax.broadcasted_iota(jnp.int32, (rows, 2 * rows), 1)
    local = lax.broadcasted_iota(jnp.int32, (rows, 2 * rows), 0)
    chosen = ((lane == local) | (lane == local + rows)).astype(BF16)
    factors = []
    for sent, d_req in zip(sents, groups, strict=True):
        table = nt_dot(chosen, sent[rows:, : 2 * rows])
        factors.append(
            [
                jnp.sum(table * serves[row : row + 1, :], axis=1, keepdims=True)
                for row in (2 * d_req, 2 * d_req + 1)
            ]
        )
    first = jnp.concatenate([pair[0] for pair in factors], axis=0)
    second = jnp.concatenate([pair[1] for pair in factors], axis=0)
    unit = lax.broadcasted_iota(jnp.int32, act.shape, 1)
    act_ref[...] = (act * jnp.where(unit < hidden, first, second)).astype(BF16)


def combine_kernel(count, groups, *refs):
    acts, near, far = refs[:count], refs[count : 2 * count], refs[2 * count : 3 * count]
    rest = refs[3 * count :]
    mixed = None
    if 0 in groups:
        mixed, rest = rest[0], rest[1:]
    rows = acts[0].shape[0] // len(groups)
    total = None
    for act, low, high in zip(acts, near, far, strict=True):
        product = nn_dot(act[...], jnp.concatenate([low[...], high[...]], axis=0))
        total = product if total is None else total + product
    for index, (d_req, out) in enumerate(zip(groups, rest, strict=True)):
        part = total[index * rows : (index + 1) * rows]
        if d_req == 0:
            part = part + mixed[...]
        out[...] = part.astype(out.dtype)


def summed_kernel(*refs):
    terms, (own_out, other_out) = refs[:-2], refs[-2:]
    _, _, core, _ = place()
    total = terms[0][...]
    for term in terms[1:]:
        total = total + term[...].astype(F32)
    block = total.shape[1] // 2
    own_out[...] = jnp.where(core == 0, total[:, :block], total[:, block:]).astype(BF16)
    other_out[...] = jnp.where(core == 0, total[:, block:], total[:, :block]).astype(BF16)


def final_kernel(own, other, out):
    _, _, core, _ = place()
    rows = own.shape[0] // 2
    for part, place_of in ((own, core), (other, 1 - core)):
        for half in range(2):
            at = pl.ds(pl.multiple_of((half * 2 + place_of) * rows, rows), rows)
            out[at, :] = part[half * rows : (half + 1) * rows, :]


def exchanged(parts, chips):
    return [
        moved(part, 0, 2 * d_row, d_exp) if d_exp or d_row else part
        for part, (d_exp, d_row) in zip(parts, chips, strict=True)
    ]


def spread(value, chips):
    return exchanged([value] * len(chips), chips)


def dense_shards(*args):
    return dense_layer(*args)


def dense_layer(
    queries,
    keys,
    values,
    lengths,
    out_weight,
    residual,
    norm_gain,
    expert_ids,
    gate_weights,
    replica_map,
    w_gate,
    w_up,
    w_down,
):
    n_req, n_kvh, n_exp = (lax.axis_size(axis) for axis in AXES)
    d_model = out_weight.shape[1]
    block = d_model // (n_kvh * n_exp)
    rows = queries.shape[0]
    n_experts = expert_ids.shape[1]
    hidden = w_gate.shape[2]
    chips = [(d_exp, d_row) for d_row in range(n_kvh // 2) for d_exp in range(n_exp)]
    n_chips = len(chips)
    gain = norm_gain.reshape(1, d_model)

    blocks = attention(chips, queries, keys, values, lengths, out_weight, w_down, block)
    down, near_weight, blocks = blocks[5:], blocks[4], list(blocks[:4])
    shares, serves = called(
        routes_kernel,
        (replica_map, expert_ids.T, gate_weights.T),
        [like((n_experts, expert_ids.shape[0]), F32), like((2 * n_req, n_experts), F32)],
        flops=0,
        n_smem=1,
    )
    blocks[3] = moved(blocks[3], 0, 1, 1)
    blocks[1] = moved(blocks[1], 0, 0, 1)
    far_weight = moved(near_weight, 0, 1, 0)
    blocks[2] = moved(blocks[2], 0, 1, 0)
    blocks[3], serves, shares = lax.optimization_barrier((blocks[3], serves, shares))
    wide = (rows, 2 * block)
    sums = called(
        lambda *refs: projection_kernel(chips, *refs),
        (*blocks, near_weight, far_weight, residual),
        [like(wide, F32)] + [like(wide, BF16)] * (n_chips - 1),
        flops=4 * rows * out_weight.size,
        scratch=[pltpu.VMEM((rows, blocks[0].shape[1]), BF16)] * 2,
    )
    w_in = [w_gate[0].T, w_up[0].T]
    later, _ = lax.optimization_barrier((tuple(w_in), sums[1]))
    w_in = [w_in[0], moved(later[0], 0, 1, 0), w_in[1], moved(later[1], 0, 1, 0)]
    down, _ = lax.optimization_barrier((tuple(down), sums[1]))
    sums = exchanged(sums, chips)
    down = exchanged(down, chips)
    down_far = [moved(piece, 0, 1, 0) for piece in down]
    mixed, sent = called(
        lambda *refs: mixed_kernel(n_chips, *refs),
        (*sums, gain, shares),
        [like(wide, F32), like((rows + n_experts, 2 * block), BF16)],
        flops=8 * rows * block,
    )
    order = range(1, n_req)
    by_group = {0: sent, **{d_req: moved(sent, d_req, 0, 0) for d_req in order}}
    half = n_req // 2
    order = [0, *order]
    terms = {}
    for groups in (tuple(order[:half]), tuple(order[half:])):
        (joined,) = called(
            joined_kernel,
            [by_group[d_req] for d_req in groups],
            [like((half * rows, 2 * block), BF16)],
            flops=0,
        )
        parts = spread(joined, chips)
        (act,) = called(
            lambda *refs, groups=groups: expert_kernel(chips, groups, *refs),
            (serves, gain, *w_in, *(by_group[d_req] for d_req in groups), *parts),
            [like((half * rows, 2 * hidden), BF16)],
            flops=8 * half * rows * d_model * hidden,
        )
        tail = (mixed,) if 0 in groups else ()
        results = called(
            lambda *refs, groups=groups: combine_kernel(n_chips, groups, *refs),
            (*spread(act, chips), *down, *down_far, *tail),
            [like(wide, F32 if d_req == 0 else BF16) for d_req in groups],
            flops=8 * half * rows * hidden * n_chips * block,
        )
        for d_req, result in zip(groups, results, strict=True):
            terms[d_req] = moved(result, d_req, 0, 0) if d_req else result
    own, other = called(
        summed_kernel,
        [terms[d_req] for d_req in order],
        [like((rows, block), BF16)] * 2,
        flops=4 * n_req * rows * block,
    )
    (out,) = called(
        final_kernel,
        (own, moved(other, 0, 1, 0)),
        [like((2 * rows, block), BF16)],
        flops=4 * rows * block,
    )
    return out


def solution(mesh):
    in_specs = (
        P(("req", "exp"), "kvh"),
        P(("req", "exp"), "kvh", None, None),
        P(("req", "exp"), "kvh", None, None),
        P("req"),
        P(("kvh", "exp"), None),
        P("req", None),
        P(),
        P("req", None),
        P("req", None),
        P(),
        P(("req", "kvh"), None, "exp"),
        P(("req", "kvh"), None, "exp"),
        P(("req", "kvh"), "exp", None),
    )
    out_specs = P("req", ("kvh", "exp"))
    sizes = tuple(mesh.shape[axis] for axis in AXES)

    def run(*args):
        dense = is_dense(sizes, args)
        step = jax.shard_map(
            dense_shards if dense else routed_shards,
            mesh=mesh,
            in_specs=in_specs,
            out_specs=out_specs,
            check_vma=False,
        )
        return step(*args)

    return run
```

```python
import jax
import jax.numpy as jnp
from jax import lax
from jax.experimental import pallas as pl
from jax.experimental.pallas import tpu as pltpu
from jax.sharding import PartitionSpec as P


def swapped(value, axis, apart):
    mask = 2**apart
    pairs = [(source, source ^ mask) for source in range(lax.axis_size(axis))]
    return lax.ppermute(value, axis, pairs)


def expert_runner(w_gate, w_up, w_down, complete, n_kvh, n_exp, block):

    def run(received):
        full = complete(received)
        lead_a = full.shape[0]
        lead_b = full.shape[1]
        d_model = w_gate.shape[1]
        rows = full.reshape(lead_a * lead_b, d_model)
        gate = jnp.dot(rows, w_gate[0], preferred_element_type=jnp.float32)
        up = jnp.dot(rows, w_up[0], preferred_element_type=jnp.float32)
        act = (jax.nn.silu(gate) * up).astype(jnp.bfloat16)
        down = jnp.dot(act, w_down[0], preferred_element_type=jnp.float32)
        terms = down.reshape(lead_a, lead_b, n_kvh, n_exp, block)
        summed = lax.psum_scatter(
            terms.astype(jnp.bfloat16), "exp", scatter_dimension=3, tiled=True
        )
        back = summed.reshape(lead_a, lead_b, n_kvh * block)
        return lax.all_to_all(back, "req", split_axis=0, concat_axis=0, tiled=True)

    return run


def routed_shards(
    queries,
    keys,
    values,
    lengths,
    out_weight,
    residual,
    norm_gain,
    expert_ids,
    gate_weights,
    replica_map,
    w_gate,
    w_up,
    w_down,
):
    f32 = jnp.float32
    half_rows_count = queries.shape[0]
    n_rows = lengths.shape[0]
    head_dim = keys.shape[3]
    span = keys.shape[2]
    heads_here = queries.shape[1] // head_dim
    n_kvh = lax.axis_size("kvh")
    n_exp = lax.axis_size("exp")
    n_req = lax.axis_size("req")
    side = lax.axis_index("exp")
    own_lengths = lax.dynamic_slice_in_dim(lengths, side * half_rows_count, half_rows_count, 0)
    query = queries.reshape(half_rows_count, heads_here, head_dim)
    scores = jnp.einsum(
        "rhd,rpd->rhp", query, keys[:, 0], preferred_element_type=f32
    ) * head_dim ** (-0.5)
    position = lax.broadcasted_iota(jnp.int32, (1, 1, span), 2)
    valid = position < own_lengths[:, None, None]
    scores = jnp.where(valid, scores, -1e30)
    peak = jnp.max(scores, axis=-1)
    weights = jnp.where(valid, jnp.exp(scores - peak[..., None]), 0.0)
    total = jnp.sum(weights, axis=-1)
    probs = weights / total[..., None]
    numer = jnp.einsum(
        "rhp,rpd->rhd", probs, values[:, 0].astype(f32), precision=lax.Precision.HIGHEST
    )
    attended_part = numer.astype(jnp.bfloat16).reshape(half_rows_count, heads_here * head_dim)
    attended = lax.all_gather(attended_part, "exp", axis=0, tiled=True)
    cut = out_weight.shape[0]
    own_heads = lax.dynamic_slice_in_dim(attended, side * cut, cut, 1)
    d_model = out_weight.shape[1]
    block = d_model // (n_kvh * n_exp)
    attn_block = (
        lax.psum_scatter(
            lax.dot_general(
                out_weight, own_heads, (((0,), (1,)), ((), ())), preferred_element_type=f32
            ).astype(jnp.bfloat16),
            ("kvh", "exp"),
            scatter_dimension=0,
            tiled=True,
        )
        .astype(jnp.float32)
        .T
    )
    offset = lax.axis_index(("kvh", "exp")) * block
    mixed = lax.dynamic_slice_in_dim(residual, offset, block, 1).astype(f32) + attn_block
    squares = lax.psum(jnp.sum(mixed * mixed, axis=1), ("kvh", "exp"))
    scale = lax.rsqrt(squares / d_model + 1e-06)
    gain_block = lax.dynamic_slice_in_dim(norm_gain, offset, block, 0)
    normed = (mixed * scale[:, None] * gain_block[None, :]).astype(jnp.bfloat16)
    top = expert_ids.shape[1]
    n_slots = replica_map.shape[0]
    n_experts = n_slots // 2
    capacity = min(n_rows, max(2, (3 * n_rows * top + 2 * n_experts - 1) // (2 * n_experts)))
    probs_top = gate_weights / jnp.sum(gate_weights, axis=1, keepdims=True)
    expert_range = jnp.arange(n_experts, dtype=jnp.int32)
    owned = (replica_map[:, None] == expert_range[None, :]).astype(jnp.int32)
    earlier = jnp.cumsum(owned, axis=0) - owned
    rank = jnp.sum(earlier * owned, axis=1)
    copies = jnp.sum(owned, axis=0)
    picked = (expert_ids[..., None] == expert_range).astype(jnp.int32)
    copies_pair = jnp.sum(picked * copies, axis=-1)
    turn = jnp.full((n_rows, top), lax.axis_index("req"), jnp.int32)
    which = turn % copies_pair
    match = (replica_map == expert_ids[..., None]) & (rank == which[..., None])
    slot = jnp.argmax(match, axis=-1)
    mine = slot % n_kvh == lax.axis_index("kvh")
    flat_dest = (slot // n_kvh).reshape(-1)
    flat_mine = mine.reshape(-1)
    toward = (
        (flat_dest[:, None] == jnp.arange(n_req, dtype=jnp.int32)[None, :]) & flat_mine[:, None]
    ).astype(jnp.int32)
    before = jnp.cumsum(toward, axis=0) - toward
    place = jnp.sum(before * toward, axis=1)
    n_buffer = n_req * capacity
    target = jnp.where(flat_mine, flat_dest * capacity + place, n_buffer)
    row_of = jnp.arange(n_rows * top, dtype=jnp.int32) // top
    source = jnp.full((n_buffer,), -1, jnp.int32).at[target].set(row_of, mode="drop")
    half_rows = lax.all_gather(normed.reshape(n_rows, 1, block), "kvh", axis=1, tiled=True).reshape(
        n_rows, n_kvh * block
    )

    def complete(received):
        partner = swapped(received, "exp", 0)
        lead_a = received.shape[0]
        lead_b = received.shape[1]
        own_part = received.reshape(lead_a, lead_b, n_kvh, 1, block)
        other_part = partner.reshape(lead_a, lead_b, n_kvh, 1, block)
        first = jnp.where(side == 0, own_part, other_part)
        second = jnp.where(side == 0, other_part, own_part)
        return jnp.concatenate([first, second], axis=3).reshape(lead_a, lead_b, n_kvh * 2 * block)

    runner = expert_runner(w_gate, w_up, w_down, complete, n_kvh, n_exp, block)
    taken = half_rows[jnp.maximum(source, 0)]
    returned = runner(
        lax.all_to_all(
            jnp.where(source[:, None] >= 0, taken, jnp.zeros((), jnp.bfloat16)).reshape(
                n_req, capacity, half_rows.shape[1]
            ),
            "req",
            split_axis=0,
            concat_axis=0,
            tiled=True,
        )
    )
    flat_back = returned.reshape(n_buffer, n_kvh * block)
    gathered = flat_back[jnp.minimum(target, n_buffer - 1)].reshape(n_rows, top, n_kvh * block)
    weight = jnp.where(mine, probs_top, 0.0)
    partial_value = jnp.zeros((n_rows, n_kvh * block), f32)
    for entry in range(top):
        partial_value = partial_value + weight[:, entry, None] * gathered[:, entry].astype(f32)
    moe_block = (
        lax.psum_scatter(
            partial_value.reshape(n_rows, n_kvh, block).astype(jnp.bfloat16),
            "kvh",
            scatter_dimension=1,
            tiled=True,
        )
        .astype(jnp.float32)
        .reshape(n_rows, block)
    )
    return (mixed + moe_block).astype(jnp.bfloat16)


F32 = jnp.float32
BF16 = jnp.bfloat16
AXES = ("req", "kvh", "exp")
STEP = 16
BATCH = 2
VMEM_LIMIT = 16 * 2**20


def is_dense(sizes, args):
    queries, keys, expert_ids, replica_map = args[0], args[1], args[7], args[9]
    n_req, n_kvh, n_exp = sizes
    span = keys.shape[2]
    rows = queries.shape[0] // (n_req * n_exp)
    powers = all(size & (size - 1) == 0 for size in (*sizes, span, rows))
    fits = n_req >= 2 and n_kvh >= 2 and n_exp == 2 and rows % (2 * STEP) == 0
    return powers and fits and expert_ids.shape[1] == replica_map.shape[0] // 2


def moved(value, d_req, d_kvh, d_exp):
    n_req, n_kvh, n_exp = (lax.axis_size(axis) for axis in AXES)
    pairs = []
    for req in range(n_req):
        for kvh in range(n_kvh):
            for exp in range(n_exp):
                source = (req * n_kvh + kvh) * n_exp + exp
                target = ((req ^ d_req) * n_kvh + (kvh ^ d_kvh)) * n_exp + (exp ^ d_exp)
                pairs.append((source, target))
    return lax.ppermute(value, AXES, pairs)


def place():
    kvh = lax.axis_index("kvh")
    return lax.axis_index("req"), kvh // 2, kvh % 2, lax.axis_index("exp")


def nt_dot(left, right, **kwargs):
    return lax.dot_general(
        left, right, (((1,), (1,)), ((), ())), preferred_element_type=F32, **kwargs
    )


def nn_dot(left, right):
    return jnp.dot(left, right, preferred_element_type=F32)


def in_vmem(count):
    return [pl.BlockSpec(memory_space=pltpu.VMEM)] * count


def in_smem():
    return pl.BlockSpec(memory_space=pltpu.SMEM)


def called(kernel, args, outs, flops, n_smem=0, scratch=()):
    moves = sum(arg.size * arg.dtype.itemsize for arg in (*args, *outs))
    return pl.pallas_call(
        kernel,
        out_shape=tuple(outs),
        in_specs=[in_smem()] * n_smem + in_vmem(len(args) - n_smem),
        out_specs=tuple(in_vmem(len(outs))),
        scratch_shapes=list(scratch),
        compiler_params=pltpu.CompilerParams(vmem_limit_bytes=VMEM_LIMIT),
        cost_estimate=pl.CostEstimate(flops=flops, bytes_accessed=moves, transcendentals=0),
    )(*args)


def like(shape, dtype):
    return jax.ShapeDtypeStruct(shape, dtype)


def attention_kernel(chips, lengths, query, key, value, weight, down, *refs):
    blocks, weight_copy, pieces = refs[:4], refs[4], refs[5:-7]
    limits, rows_ref, wide_ref, done_ref, key_ref, value_ref, sems = refs[-7:]
    _, _, core, side = place()
    n_rows = query.shape[0]
    span, head_dim = key.shape[2], key.shape[3]
    heads = query.shape[1] // head_dim
    n = STEP
    steps = n_rows // n

    def cached(step, index):
        source, target = ((key, key_ref), (value, value_ref))[index]
        here = pl.ds(step * n, n)
        return pltpu.make_async_copy(source.at[here], target.at[here], sems.at[2 * step + index])

    begin = [
        pltpu.make_async_copy(query, rows_ref, sems.at[2 * steps]),
        pltpu.make_async_copy(lengths, limits, sems.at[2 * steps + 1]),
    ]
    rest = [pltpu.make_async_copy(weight, weight_copy, sems.at[2 * steps + 2])]
    block = pieces[0].shape[1] // 2
    for piece, (d_exp, d_row) in zip(pieces, chips, strict=True):
        for index in range(2):
            source = down.at[0, :, pl.ds(columns_of(d_exp, d_row, index, block), block)]
            target = piece.at[:, index * block : (index + 1) * block]
            sem = sems.at[2 * steps + 2 + len(rest)]
            rest.append(pltpu.make_async_copy(source, target, sem))
    for copy in begin:
        copy.start()
    for step in range(steps):
        for index in range(2):
            cached(step, index).start()
    for copy in rest:
        copy.start()
    column = lax.broadcasted_iota(jnp.int32, (1, n * span), 1)
    owner = lax.shift_right_logical(column, span.bit_length() - 1)
    position = column & (span - 1)
    request = lax.broadcasted_iota(jnp.int32, (heads * n, 1), 0) & (n - 1)
    same = request == owner
    for copy in begin:
        copy.wait()
    wide_ref[...] = rows_ref[...].astype(F32)

    for batch in range(0, steps, BATCH):
        batch_steps = range(batch, batch + BATCH)
        masked = []
        for step in batch_steps:
            here = slice(step * n, (step + 1) * n)
            rows = jnp.concatenate(
                [wide_ref[here, head * head_dim : (head + 1) * head_dim] for head in range(heads)],
                axis=0,
            ).astype(BF16)
            limit = jnp.zeros((1, n * span), jnp.int32)
            first = side * n_rows + step * n
            for index in range(n):
                limit = jnp.where(owner == index, limits[first + index], limit)
            valid = same & (position < limit)
            if step == batch:
                for ahead in batch_steps:
                    cached(ahead, 0).wait()
                    cached(ahead, 1).wait()
            scores = nt_dot(rows, key_ref[here].reshape(n * span, head_dim)) * head_dim ** (-0.5)
            masked.append(jnp.where(valid, scores, -1e30))
        scores = jnp.concatenate(masked, axis=0)
        peak = jnp.max(scores, axis=1, keepdims=True)
        weights = jnp.exp(scores - peak)
        total = jnp.sum(weights, axis=1, keepdims=True)
        high = weights.astype(BF16)
        low = (weights - high.astype(F32)).astype(BF16)
        for step in batch_steps:
            here = slice(step * n, (step + 1) * n)
            own = slice((step - batch) * heads * n, (step - batch + 1) * heads * n)
            held = value_ref[here].reshape(n * span, head_dim)
            both = nn_dot(jnp.concatenate([high[own], low[own]], axis=0), held)
            numer = (both[: heads * n] + both[heads * n :]) / total[own]
            for head in range(heads):
                done_ref[here, head * head_dim : (head + 1) * head_dim] = numer[
                    head * n : (head + 1) * n
                ]

    half, width = n_rows // 2, query.shape[1] // 2
    for index, out in enumerate(blocks):
        at = core if index < 2 else 1 - core
        towards = side if index % 2 == 0 else 1 - side
        spot = pl.ds(pl.multiple_of(at * half, half), half)
        out[...] = done_ref[spot, pl.ds(pl.multiple_of(towards * width, width), width)].astype(BF16)
    for copy in rest:
        copy.wait()


def attention(chips, queries, keys, values, lengths, out_weight, w_down, block):
    rows = queries.shape[0]
    span = keys.shape[2]
    piece = like((rows // 2, queries.shape[1] // 2), BF16)
    args = (lengths, queries, keys, values, out_weight, w_down)
    outs = [piece] * 4 + [like(out_weight.shape, BF16)]
    outs += [like((w_down.shape[1], 2 * block), BF16)] * len(chips)
    return pl.pallas_call(
        lambda *refs: attention_kernel(chips, *refs),
        out_shape=tuple(outs),
        in_specs=[pl.BlockSpec(memory_space=pltpu.HBM)] * len(args),
        out_specs=tuple(in_vmem(len(outs))),
        scratch_shapes=[
            pltpu.SMEM(lengths.shape, jnp.int32),
            pltpu.VMEM(queries.shape, BF16),
            pltpu.VMEM(queries.shape, F32),
            pltpu.VMEM(queries.shape, F32),
            pltpu.VMEM(keys.shape, BF16),
            pltpu.VMEM(values.shape, BF16),
            pltpu.SemaphoreType.DMA((3 + 2 * (rows // STEP) + 2 * len(chips),)),
        ],
        cost_estimate=pl.CostEstimate(
            flops=6 * STEP * rows * queries.shape[1] * span,
            bytes_accessed=2 * keys.size * 2,
            transcendentals=0,
        ),
        compiler_params=pltpu.CompilerParams(vmem_limit_bytes=VMEM_LIMIT),
        name="attention",
    )(*(pltpu.with_memory_space_constraint(arg, pltpu.HBM) for arg in args))


def routes_kernel(slots, ids, gates, shares, serves):
    probs_top = gates[...] / jnp.sum(gates[...], axis=0, keepdims=True)
    n_experts = shares.shape[0]
    for expert in range(n_experts):
        shares[expert : expert + 1, :] = jnp.sum(
            jnp.where(ids[...] == expert, probs_top, 0.0), axis=0, keepdims=True
        )
    req, row, core, _ = place()
    n_kvh = lax.axis_size("kvh")
    lane = lax.broadcasted_iota(jnp.int32, (1, n_experts), 1)
    n_req = serves.shape[0] // 2
    for index, at in enumerate((core, 1 - core)):
        slot = req * n_kvh + row * 2 + at
        expert = slots[slot]
        copies = jnp.int32(0)
        rank = jnp.int32(0)
        for other in range(slots.shape[0]):
            same = (slots[other] == expert).astype(jnp.int32)
            copies = copies + same
            rank = rank + jnp.where(other < slot, same, 0)
        for d_req in range(n_req):
            chosen = jnp.where(lax.rem(req ^ d_req, copies) == rank, expert, -1)
            serves[2 * d_req + index : 2 * d_req + index + 1, :] = (lane == chosen).astype(F32)


def columns_of(d_exp, d_row, index, block):
    _, row, _, side = place()
    return pl.multiple_of((((row ^ d_row) * 2 + index) * 2 + (side ^ d_exp)) * block, block)


def projection_kernel(chips, *refs):
    pieces, (near_weight, far_weight, residual), outs = refs[:4], refs[4:7], refs[7:-2]
    near, far = refs[-2:]
    _, _, core, side = place()
    rows = pieces[0].shape[0]
    block = outs[0].shape[1] // 2
    spots = [pl.ds(pl.multiple_of((side ^ d) * rows, rows), rows) for d in range(2)]
    for d in range(2):
        near[spots[d], :] = pieces[d][...]
        far[spots[d], :] = pieces[2 + d][...]
    for chip, (d_exp, d_row) in enumerate(chips):
        for index in range(2):
            start = columns_of(d_exp, d_row, index, block)
            where = pl.ds(start, block)
            part = nn_dot(near[...], near_weight[:, where]) + nn_dot(far[...], far_weight[:, where])
            here = slice(index * block, (index + 1) * block)
            if chip:
                outs[chip][:, here] = part.astype(BF16)
                continue
            for half in range(2):
                own = slice(half * rows, (half + 1) * rows)
                at = pl.ds(pl.multiple_of((half * 2 + core) * rows, rows), rows)
                outs[0][own, here] = part[own] + residual[at, where].astype(F32)


def own_tokens(rows, n_tokens, core):
    half = rows // 2
    local = lax.broadcasted_iota(jnp.int32, (rows, 1), 0)
    token = local + jnp.where(local >= half, half, 0) + core * half
    lane = lax.broadcasted_iota(jnp.int32, (rows, n_tokens), 1)
    return (lane == token).astype(F32)


def mixed_kernel(count, *refs):
    own, others, (gain, shares, mixed, sent) = refs[0], refs[1:count], refs[count:]
    rows = own.shape[0]
    block = own.shape[1] // 2
    _, _, core, _ = place()
    for index in range(2):
        here = slice(index * block, (index + 1) * block)
        total = own[:, here]
        for other in others:
            total = total + other[:, here].astype(F32)
        mixed[:, here] = total
        scale = gain[:, pl.ds(columns_of(0, 0, index, block), block)]
        sent[:rows, here] = (total * scale).astype(BF16)
    chosen = own_tokens(rows, shares.shape[1], core)
    table = nt_dot(shares[...], chosen, precision=lax.Precision.HIGHEST)
    high = table.astype(BF16)
    low = (table - high.astype(F32)).astype(BF16)
    rest = jnp.zeros((table.shape[0], 2 * block - 2 * rows), BF16)
    sent[rows:, :] = jnp.concatenate([high, low, rest], axis=1)


def joined_kernel(*refs):
    out = refs[-1]
    rows = out.shape[0] // (len(refs) - 1)
    for index, ref in enumerate(refs[:-1]):
        out[index * rows : (index + 1) * rows, :] = ref[:rows, :]


def expert_kernel(chips, groups, *refs):
    serves, gain = refs[0], refs[1]
    weights = refs[2:6]
    sents = refs[6 : 6 + len(groups)]
    parts = refs[6 + len(groups) : -1]
    act_ref = refs[-1]
    rows = parts[0].shape[0] // len(groups)
    block = parts[0].shape[1] // 2
    hidden, d_model = weights[0].shape
    gates = None
    squares = None
    for part_ref, (d_exp, d_row) in zip(parts, chips, strict=True):
        for index in range(2):
            where = pl.ds(columns_of(d_exp, d_row, index, block), block)
            part = part_ref[:, index * block : (index + 1) * block]
            weight = jnp.concatenate([ref[:, where] for ref in weights], axis=0)
            product = nt_dot(part, weight)
            plain = part.astype(F32)
            scale = gain[:, where]
            square = jnp.sum(plain * plain * (1.0 / (scale * scale)), axis=1, keepdims=True)
            gates = product if gates is None else gates + product
            squares = square if squares is None else squares + square
    scale = lax.rsqrt(squares / d_model + 1e-06)
    gate = gates[:, : 2 * hidden] * scale
    up = gates[:, 2 * hidden :] * scale
    act = gate / (1.0 + jnp.exp(-gate)) * up
    lane = lax.broadcasted_iota(jnp.int32, (rows, 2 * rows), 1)
    local = lax.broadcasted_iota(jnp.int32, (rows, 2 * rows), 0)
    chosen = ((lane == local) | (lane == local + rows)).astype(BF16)
    factors = []
    for sent, d_req in zip(sents, groups, strict=True):
        table = nt_dot(chosen, sent[rows:, : 2 * rows])
        factors.append(
            [
                jnp.sum(table * serves[row : row + 1, :], axis=1, keepdims=True)
                for row in (2 * d_req, 2 * d_req + 1)
            ]
        )
    first = jnp.concatenate([pair[0] for pair in factors], axis=0)
    second = jnp.concatenate([pair[1] for pair in factors], axis=0)
    unit = lax.broadcasted_iota(jnp.int32, act.shape, 1)
    act_ref[...] = (act * jnp.where(unit < hidden, first, second)).astype(BF16)


def combine_kernel(count, groups, *refs):
    acts, near, far = refs[:count], refs[count : 2 * count], refs[2 * count : 3 * count]
    rest = refs[3 * count :]
    mixed = None
    if 0 in groups:
        mixed, rest = rest[0], rest[1:]
    rows = acts[0].shape[0] // len(groups)
    total = None
    for act, low, high in zip(acts, near, far, strict=True):
        product = nn_dot(act[...], jnp.concatenate([low[...], high[...]], axis=0))
        total = product if total is None else total + product
    for index, (d_req, out) in enumerate(zip(groups, rest, strict=True)):
        part = total[index * rows : (index + 1) * rows]
        if d_req == 0:
            part = part + mixed[...]
        out[...] = part.astype(out.dtype)


def summed_kernel(*refs):
    terms, (own_out, other_out) = refs[:-2], refs[-2:]
    _, _, core, _ = place()
    total = terms[0][...]
    for term in terms[1:]:
        total = total + term[...].astype(F32)
    block = total.shape[1] // 2
    own_out[...] = jnp.where(core == 0, total[:, :block], total[:, block:]).astype(BF16)
    other_out[...] = jnp.where(core == 0, total[:, block:], total[:, :block]).astype(BF16)


def final_kernel(own, other, out):
    _, _, core, _ = place()
    rows = own.shape[0] // 2
    for part, place_of in ((own, core), (other, 1 - core)):
        for half in range(2):
            at = pl.ds(pl.multiple_of((half * 2 + place_of) * rows, rows), rows)
            out[at, :] = part[half * rows : (half + 1) * rows, :]


def exchanged(parts, chips):
    return [
        moved(part, 0, 2 * d_row, d_exp) if d_exp or d_row else part
        for part, (d_exp, d_row) in zip(parts, chips, strict=True)
    ]


def spread(value, chips):
    return exchanged([value] * len(chips), chips)


def dense_shards(*args):
    return dense_layer(*args)


def dense_layer(
    queries,
    keys,
    values,
    lengths,
    out_weight,
    residual,
    norm_gain,
    expert_ids,
    gate_weights,
    replica_map,
    w_gate,
    w_up,
    w_down,
):
    n_req, n_kvh, n_exp = (lax.axis_size(axis) for axis in AXES)
    d_model = out_weight.shape[1]
    block = d_model // (n_kvh * n_exp)
    rows = queries.shape[0]
    n_experts = expert_ids.shape[1]
    hidden = w_gate.shape[2]
    chips = [(d_exp, d_row) for d_row in range(n_kvh // 2) for d_exp in range(n_exp)]
    n_chips = len(chips)
    gain = norm_gain.reshape(1, d_model)

    blocks = attention(chips, queries, keys, values, lengths, out_weight, w_down, block)
    down, near_weight, blocks = blocks[5:], blocks[4], list(blocks[:4])
    shares, serves = called(
        routes_kernel,
        (replica_map, expert_ids.T, gate_weights.T),
        [like((n_experts, expert_ids.shape[0]), F32), like((2 * n_req, n_experts), F32)],
        flops=0,
        n_smem=1,
    )
    blocks[3] = moved(blocks[3], 0, 1, 1)
    blocks[1] = moved(blocks[1], 0, 0, 1)
    far_weight = moved(near_weight, 0, 1, 0)
    blocks[2] = moved(blocks[2], 0, 1, 0)
    blocks[3], serves, shares = lax.optimization_barrier((blocks[3], serves, shares))
    wide = (rows, 2 * block)
    sums = called(
        lambda *refs: projection_kernel(chips, *refs),
        (*blocks, near_weight, far_weight, residual),
        [like(wide, F32)] + [like(wide, BF16)] * (n_chips - 1),
        flops=4 * rows * out_weight.size,
        scratch=[pltpu.VMEM((rows, blocks[0].shape[1]), BF16)] * 2,
    )
    w_in = [w_gate[0].T, w_up[0].T]
    later, _ = lax.optimization_barrier((tuple(w_in), sums[1]))
    w_in = [w_in[0], moved(later[0], 0, 1, 0), w_in[1], moved(later[1], 0, 1, 0)]
    down, _ = lax.optimization_barrier((tuple(down), sums[1]))
    sums = exchanged(sums, chips)
    down = exchanged(down, chips)
    down_far = [moved(piece, 0, 1, 0) for piece in down]
    mixed, sent = called(
        lambda *refs: mixed_kernel(n_chips, *refs),
        (*sums, gain, shares),
        [like(wide, F32), like((rows + n_experts, 2 * block), BF16)],
        flops=8 * rows * block,
    )
    order = range(1, n_req)
    by_group = {0: sent, **{d_req: moved(sent, d_req, 0, 0) for d_req in order}}
    half = n_req // 2
    order = [0, *order]
    terms = {}
    for groups in (tuple(order[:half]), tuple(order[half:])):
        (joined,) = called(
            joined_kernel,
            [by_group[d_req] for d_req in groups],
            [like((half * rows, 2 * block), BF16)],
            flops=0,
        )
        parts = spread(joined, chips)
        (act,) = called(
            lambda *refs, groups=groups: expert_kernel(chips, groups, *refs),
            (serves, gain, *w_in, *(by_group[d_req] for d_req in groups), *parts),
            [like((half * rows, 2 * hidden), BF16)],
            flops=8 * half * rows * d_model * hidden,
        )
        tail = (mixed,) if 0 in groups else ()
        results = called(
            lambda *refs, groups=groups: combine_kernel(n_chips, groups, *refs),
            (*spread(act, chips), *down, *down_far, *tail),
            [like(wide, F32 if d_req == 0 else BF16) for d_req in groups],
            flops=8 * half * rows * hidden * n_chips * block,
        )
        for d_req, result in zip(groups, results, strict=True):
            terms[d_req] = moved(result, d_req, 0, 0) if d_req else result
    own, other = called(
        summed_kernel,
        [terms[d_req] for d_req in order],
        [like((rows, block), BF16)] * 2,
        flops=4 * n_req * rows * block,
    )
    (out,) = called(
        final_kernel,
        (own, moved(other, 0, 1, 0)),
        [like((2 * rows, block), BF16)],
        flops=4 * rows * block,
    )
    return out


def solution(mesh):
    in_specs = (
        P(("req", "exp"), "kvh"),
        P(("req", "exp"), "kvh", None, None),
        P(("req", "exp"), "kvh", None, None),
        P("req"),
        P(("kvh", "exp"), None),
        P("req", None),
        P(),
        P("req", None),
        P("req", None),
        P(),
        P(("req", "kvh"), None, "exp"),
        P(("req", "kvh"), None, "exp"),
        P(("req", "kvh"), "exp", None),
    )
    out_specs = P("req", ("kvh", "exp"))
    sizes = tuple(mesh.shape[axis] for axis in AXES)

    def run(*args):
        dense = is_dense(sizes, args)
        step = jax.shard_map(
            dense_shards if dense else routed_shards,
            mesh=mesh,
            in_specs=in_specs,
            out_specs=out_specs,
            check_vma=False,
        )
        return step(*args)

    return run
```

```python
import jax
import jax.numpy as jnp
from jax import lax
from jax.experimental import pallas as pl
from jax.experimental.pallas import tpu as pltpu
from jax.sharding import PartitionSpec as P


def swapped(value, axis, apart):
    mask = 2**apart
    pairs = [(source, source ^ mask) for source in range(lax.axis_size(axis))]
    return lax.ppermute(value, axis, pairs)


def expert_runner(w_gate, w_up, w_down, complete, n_kvh, n_exp, block):

    def run(received):
        full = complete(received)
        lead_a = full.shape[0]
        lead_b = full.shape[1]
        d_model = w_gate.shape[1]
        rows = full.reshape(lead_a * lead_b, d_model)
        gate = jnp.dot(rows, w_gate[0], preferred_element_type=jnp.float32)
        up = jnp.dot(rows, w_up[0], preferred_element_type=jnp.float32)
        act = (jax.nn.silu(gate) * up).astype(jnp.bfloat16)
        down = jnp.dot(act, w_down[0], preferred_element_type=jnp.float32)
        terms = down.reshape(lead_a, lead_b, n_kvh, n_exp, block)
        summed = lax.psum_scatter(
            terms.astype(jnp.bfloat16), "exp", scatter_dimension=3, tiled=True
        )
        back = summed.reshape(lead_a, lead_b, n_kvh * block)
        return lax.all_to_all(back, "req", split_axis=0, concat_axis=0, tiled=True)

    return run


def routed_shards(
    queries,
    keys,
    values,
    lengths,
    out_weight,
    residual,
    norm_gain,
    expert_ids,
    gate_weights,
    replica_map,
    w_gate,
    w_up,
    w_down,
):
    f32 = jnp.float32
    half_rows_count = queries.shape[0]
    n_rows = lengths.shape[0]
    head_dim = keys.shape[3]
    span = keys.shape[2]
    heads_here = queries.shape[1] // head_dim
    n_kvh = lax.axis_size("kvh")
    n_exp = lax.axis_size("exp")
    n_req = lax.axis_size("req")
    side = lax.axis_index("exp")
    own_lengths = lax.dynamic_slice_in_dim(lengths, side * half_rows_count, half_rows_count, 0)
    query = queries.reshape(half_rows_count, heads_here, head_dim)
    scores = jnp.einsum(
        "rhd,rpd->rhp", query, keys[:, 0], preferred_element_type=f32
    ) * head_dim ** (-0.5)
    position = lax.broadcasted_iota(jnp.int32, (1, 1, span), 2)
    valid = position < own_lengths[:, None, None]
    scores = jnp.where(valid, scores, -1e30)
    peak = jnp.max(scores, axis=-1)
    weights = jnp.where(valid, jnp.exp(scores - peak[..., None]), 0.0)
    total = jnp.sum(weights, axis=-1)
    probs = weights / total[..., None]
    numer = jnp.einsum(
        "rhp,rpd->rhd", probs, values[:, 0].astype(f32), precision=lax.Precision.HIGHEST
    )
    attended_part = numer.astype(jnp.bfloat16).reshape(half_rows_count, heads_here * head_dim)
    attended = lax.all_gather(attended_part, "exp", axis=0, tiled=True)
    cut = out_weight.shape[0]
    own_heads = lax.dynamic_slice_in_dim(attended, side * cut, cut, 1)
    d_model = out_weight.shape[1]
    block = d_model // (n_kvh * n_exp)
    attn_block = (
        lax.psum_scatter(
            lax.dot_general(
                out_weight, own_heads, (((0,), (1,)), ((), ())), preferred_element_type=f32
            ).astype(jnp.bfloat16),
            ("kvh", "exp"),
            scatter_dimension=0,
            tiled=True,
        )
        .astype(jnp.float32)
        .T
    )
    offset = lax.axis_index(("kvh", "exp")) * block
    mixed = lax.dynamic_slice_in_dim(residual, offset, block, 1).astype(f32) + attn_block
    squares = lax.psum(jnp.sum(mixed * mixed, axis=1), ("kvh", "exp"))
    scale = lax.rsqrt(squares / d_model + 1e-06)
    gain_block = lax.dynamic_slice_in_dim(norm_gain, offset, block, 0)
    normed = (mixed * scale[:, None] * gain_block[None, :]).astype(jnp.bfloat16)
    top = expert_ids.shape[1]
    n_slots = replica_map.shape[0]
    n_experts = n_slots // 2
    capacity = min(n_rows, max(2, (3 * n_rows * top + 2 * n_experts - 1) // (2 * n_experts)))
    probs_top = gate_weights / jnp.sum(gate_weights, axis=1, keepdims=True)
    expert_range = jnp.arange(n_experts, dtype=jnp.int32)
    owned = (replica_map[:, None] == expert_range[None, :]).astype(jnp.int32)
    earlier = jnp.cumsum(owned, axis=0) - owned
    rank = jnp.sum(earlier * owned, axis=1)
    copies = jnp.sum(owned, axis=0)
    picked = (expert_ids[..., None] == expert_range).astype(jnp.int32)
    copies_pair = jnp.sum(picked * copies, axis=-1)
    turn = jnp.full((n_rows, top), lax.axis_index("req"), jnp.int32)
    which = turn % copies_pair
    match = (replica_map == expert_ids[..., None]) & (rank == which[..., None])
    slot = jnp.argmax(match, axis=-1)
    mine = slot % n_kvh == lax.axis_index("kvh")
    flat_dest = (slot // n_kvh).reshape(-1)
    flat_mine = mine.reshape(-1)
    toward = (
        (flat_dest[:, None] == jnp.arange(n_req, dtype=jnp.int32)[None, :]) & flat_mine[:, None]
    ).astype(jnp.int32)
    before = jnp.cumsum(toward, axis=0) - toward
    place = jnp.sum(before * toward, axis=1)
    n_buffer = n_req * capacity
    target = jnp.where(flat_mine, flat_dest * capacity + place, n_buffer)
    row_of = jnp.arange(n_rows * top, dtype=jnp.int32) // top
    source = jnp.full((n_buffer,), -1, jnp.int32).at[target].set(row_of, mode="drop")
    half_rows = lax.all_gather(normed.reshape(n_rows, 1, block), "kvh", axis=1, tiled=True).reshape(
        n_rows, n_kvh * block
    )

    def complete(received):
        partner = swapped(received, "exp", 0)
        lead_a = received.shape[0]
        lead_b = received.shape[1]
        own_part = received.reshape(lead_a, lead_b, n_kvh, 1, block)
        other_part = partner.reshape(lead_a, lead_b, n_kvh, 1, block)
        first = jnp.where(side == 0, own_part, other_part)
        second = jnp.where(side == 0, other_part, own_part)
        return jnp.concatenate([first, second], axis=3).reshape(lead_a, lead_b, n_kvh * 2 * block)

    runner = expert_runner(w_gate, w_up, w_down, complete, n_kvh, n_exp, block)
    taken = half_rows[jnp.maximum(source, 0)]
    returned = runner(
        lax.all_to_all(
            jnp.where(source[:, None] >= 0, taken, jnp.zeros((), jnp.bfloat16)).reshape(
                n_req, capacity, half_rows.shape[1]
            ),
            "req",
            split_axis=0,
            concat_axis=0,
            tiled=True,
        )
    )
    flat_back = returned.reshape(n_buffer, n_kvh * block)
    gathered = flat_back[jnp.minimum(target, n_buffer - 1)].reshape(n_rows, top, n_kvh * block)
    weight = jnp.where(mine, probs_top, 0.0)
    partial_value = jnp.zeros((n_rows, n_kvh * block), f32)
    for entry in range(top):
        partial_value = partial_value + weight[:, entry, None] * gathered[:, entry].astype(f32)
    moe_block = (
        lax.psum_scatter(
            partial_value.reshape(n_rows, n_kvh, block).astype(jnp.bfloat16),
            "kvh",
            scatter_dimension=1,
            tiled=True,
        )
        .astype(jnp.float32)
        .reshape(n_rows, block)
    )
    return (mixed + moe_block).astype(jnp.bfloat16)


F32 = jnp.float32
BF16 = jnp.bfloat16
AXES = ("req", "kvh", "exp")
STEP = 16
BATCH = 2
VMEM_LIMIT = 16 * 2**20


def is_dense(sizes, args):
    queries, keys, expert_ids, replica_map = args[0], args[1], args[7], args[9]
    n_req, n_kvh, n_exp = sizes
    span = keys.shape[2]
    rows = queries.shape[0] // (n_req * n_exp)
    powers = all(size & (size - 1) == 0 for size in (*sizes, span, rows))
    fits = n_req >= 2 and n_kvh >= 2 and n_exp == 2 and rows % (2 * STEP) == 0
    return powers and fits and expert_ids.shape[1] == replica_map.shape[0] // 2


def moved(value, d_req, d_kvh, d_exp):
    n_req, n_kvh, n_exp = (lax.axis_size(axis) for axis in AXES)
    pairs = []
    for req in range(n_req):
        for kvh in range(n_kvh):
            for exp in range(n_exp):
                source = (req * n_kvh + kvh) * n_exp + exp
                target = ((req ^ d_req) * n_kvh + (kvh ^ d_kvh)) * n_exp + (exp ^ d_exp)
                pairs.append((source, target))
    return lax.ppermute(value, AXES, pairs)


def place():
    kvh = lax.axis_index("kvh")
    return lax.axis_index("req"), kvh // 2, kvh % 2, lax.axis_index("exp")


def nt_dot(left, right, **kwargs):
    return lax.dot_general(
        left, right, (((1,), (1,)), ((), ())), preferred_element_type=F32, **kwargs
    )


def nn_dot(left, right):
    return jnp.dot(left, right, preferred_element_type=F32)


def in_vmem(count):
    return [pl.BlockSpec(memory_space=pltpu.VMEM)] * count


def in_smem():
    return pl.BlockSpec(memory_space=pltpu.SMEM)


def called(kernel, args, outs, flops, n_smem=0, scratch=()):
    moves = sum(arg.size * arg.dtype.itemsize for arg in (*args, *outs))
    return pl.pallas_call(
        kernel,
        out_shape=tuple(outs),
        in_specs=[in_smem()] * n_smem + in_vmem(len(args) - n_smem),
        out_specs=tuple(in_vmem(len(outs))),
        scratch_shapes=list(scratch),
        compiler_params=pltpu.CompilerParams(vmem_limit_bytes=VMEM_LIMIT),
        cost_estimate=pl.CostEstimate(flops=flops, bytes_accessed=moves, transcendentals=0),
    )(*args)


def like(shape, dtype):
    return jax.ShapeDtypeStruct(shape, dtype)


def attention_kernel(chips, lengths, query, key, value, weight, down, *refs):
    blocks, weight_copy, pieces = refs[:4], refs[4], refs[5:-7]
    limits, rows_ref, wide_ref, done_ref, key_ref, value_ref, sems = refs[-7:]
    _, _, core, side = place()
    n_rows = query.shape[0]
    span, head_dim = key.shape[2], key.shape[3]
    heads = query.shape[1] // head_dim
    n = STEP
    steps = n_rows // n

    def cached(step, index):
        source, target = ((key, key_ref), (value, value_ref))[index]
        here = pl.ds(step * n, n)
        return pltpu.make_async_copy(source.at[here], target.at[here], sems.at[2 * step + index])

    begin = [
        pltpu.make_async_copy(query, rows_ref, sems.at[2 * steps]),
        pltpu.make_async_copy(lengths, limits, sems.at[2 * steps + 1]),
    ]
    rest = [pltpu.make_async_copy(weight, weight_copy, sems.at[2 * steps + 2])]
    block = pieces[0].shape[1] // 2
    for piece, (d_exp, d_row) in zip(pieces, chips, strict=True):
        for index in range(2):
            source = down.at[0, :, pl.ds(columns_of(d_exp, d_row, index, block), block)]
            target = piece.at[:, index * block : (index + 1) * block]
            sem = sems.at[2 * steps + 2 + len(rest)]
            rest.append(pltpu.make_async_copy(source, target, sem))
    for copy in begin:
        copy.start()
    for step in range(steps):
        for index in range(2):
            cached(step, index).start()
    for copy in rest:
        copy.start()
    column = lax.broadcasted_iota(jnp.int32, (1, n * span), 1)
    owner = lax.shift_right_logical(column, span.bit_length() - 1)
    position = column & (span - 1)
    request = lax.broadcasted_iota(jnp.int32, (heads * n, 1), 0) & (n - 1)
    same = request == owner
    for copy in begin:
        copy.wait()
    wide_ref[...] = rows_ref[...].astype(F32)

    for batch in range(0, steps, BATCH):
        batch_steps = range(batch, batch + BATCH)
        masked = []
        for step in batch_steps:
            here = slice(step * n, (step + 1) * n)
            rows = jnp.concatenate(
                [wide_ref[here, head * head_dim : (head + 1) * head_dim] for head in range(heads)],
                axis=0,
            ).astype(BF16)
            limit = jnp.zeros((1, n * span), jnp.int32)
            first = side * n_rows + step * n
            for index in range(n):
                limit = jnp.where(owner == index, limits[first + index], limit)
            valid = same & (position < limit)
            if step == batch:
                for ahead in batch_steps:
                    cached(ahead, 0).wait()
                    cached(ahead, 1).wait()
            scores = nt_dot(rows, key_ref[here].reshape(n * span, head_dim)) * head_dim ** (-0.5)
            masked.append(jnp.where(valid, scores, -1e30))
        scores = jnp.concatenate(masked, axis=0)
        peak = jnp.max(scores, axis=1, keepdims=True)
        weights = jnp.exp(scores - peak)
        total = jnp.sum(weights, axis=1, keepdims=True)
        high = weights.astype(BF16)
        low = (weights - high.astype(F32)).astype(BF16)
        for step in batch_steps:
            here = slice(step * n, (step + 1) * n)
            own = slice((step - batch) * heads * n, (step - batch + 1) * heads * n)
            held = value_ref[here].reshape(n * span, head_dim)
            both = nn_dot(jnp.concatenate([high[own], low[own]], axis=0), held)
            numer = (both[: heads * n] + both[heads * n :]) / total[own]
            for head in range(heads):
                done_ref[here, head * head_dim : (head + 1) * head_dim] = numer[
                    head * n : (head + 1) * n
                ]

    half, width = n_rows // 2, query.shape[1] // 2
    for index, out in enumerate(blocks):
        at = core if index < 2 else 1 - core
        towards = side if index % 2 == 0 else 1 - side
        spot = pl.ds(pl.multiple_of(at * half, half), half)
        out[...] = done_ref[spot, pl.ds(pl.multiple_of(towards * width, width), width)].astype(BF16)
    for copy in rest:
        copy.wait()


def attention(chips, queries, keys, values, lengths, out_weight, w_down, block):
    rows = queries.shape[0]
    span = keys.shape[2]
    piece = like((rows // 2, queries.shape[1] // 2), BF16)
    args = (lengths, queries, keys, values, out_weight, w_down)
    outs = [piece] * 4 + [like(out_weight.shape, BF16)]
    outs += [like((w_down.shape[1], 2 * block), BF16)] * len(chips)
    return pl.pallas_call(
        lambda *refs: attention_kernel(chips, *refs),
        out_shape=tuple(outs),
        in_specs=[pl.BlockSpec(memory_space=pltpu.HBM)] * len(args),
        out_specs=tuple(in_vmem(len(outs))),
        scratch_shapes=[
            pltpu.SMEM(lengths.shape, jnp.int32),
            pltpu.VMEM(queries.shape, BF16),
            pltpu.VMEM(queries.shape, F32),
            pltpu.VMEM(queries.shape, F32),
            pltpu.VMEM(keys.shape, BF16),
            pltpu.VMEM(values.shape, BF16),
            pltpu.SemaphoreType.DMA((3 + 2 * (rows // STEP) + 2 * len(chips),)),
        ],
        cost_estimate=pl.CostEstimate(
            flops=6 * STEP * rows * queries.shape[1] * span,
            bytes_accessed=2 * keys.size * 2,
            transcendentals=0,
        ),
        compiler_params=pltpu.CompilerParams(vmem_limit_bytes=VMEM_LIMIT),
        name="attention",
    )(*(pltpu.with_memory_space_constraint(arg, pltpu.HBM) for arg in args))


def routes_kernel(rows, slots, ids, gates, gate, up, tail, serves, weights, sems):
    hidden = gate.shape[0]
    copies_in = [
        pltpu.make_async_copy(ref, weights.at[index * hidden : (index + 1) * hidden, :], sems.at[index])
        for index, ref in enumerate((gate, up))
    ]
    for copy in copies_in:
        copy.start()
    probs_top = gates[...] / jnp.sum(gates[...], axis=0, keepdims=True)
    n_experts, width = tail.shape
    shares = jnp.concatenate(
        [
            jnp.sum(jnp.where(ids[...] == expert, probs_top, 0.0), axis=0, keepdims=True)
            for expert in range(n_experts)
        ],
        axis=0,
    )
    chosen = own_tokens(rows, shares.shape[1], place()[2])
    table = nt_dot(shares, chosen, precision=lax.Precision.HIGHEST)
    high = table.astype(BF16)
    low = (table - high.astype(F32)).astype(BF16)
    rest = jnp.zeros((n_experts, width - 2 * rows), BF16)
    tail[...] = jnp.concatenate([high, low, rest], axis=1)
    req, row, core, _ = place()
    n_kvh = lax.axis_size("kvh")
    lane = lax.broadcasted_iota(jnp.int32, (1, n_experts), 1)
    n_req = serves.shape[0] // 2
    for index, at in enumerate((core, 1 - core)):
        slot = req * n_kvh + row * 2 + at
        expert = slots[slot]
        copies = jnp.int32(0)
        rank = jnp.int32(0)
        for other in range(slots.shape[0]):
            same = (slots[other] == expert).astype(jnp.int32)
            copies = copies + same
            rank = rank + jnp.where(other < slot, same, 0)
        for d_req in range(n_req):
            chosen = jnp.where(lax.rem(req ^ d_req, copies) == rank, expert, -1)
            serves[2 * d_req + index : 2 * d_req + index + 1, :] = (lane == chosen).astype(F32)
    for copy in copies_in:
        copy.wait()


def columns_of(d_exp, d_row, index, block):
    _, row, _, side = place()
    return pl.multiple_of((((row ^ d_row) * 2 + index) * 2 + (side ^ d_exp)) * block, block)


def projection_kernel(chips, *refs):
    pieces, (near_weight, far_weight, residual), outs = refs[:4], refs[4:7], refs[7:-2]
    near, far = refs[-2:]
    _, _, core, side = place()
    rows = pieces[0].shape[0]
    block = outs[0].shape[1] // 2
    spots = [pl.ds(pl.multiple_of((side ^ d) * rows, rows), rows) for d in range(2)]
    for d in range(2):
        near[spots[d], :] = pieces[d][...]
        far[spots[d], :] = pieces[2 + d][...]
    for chip, (d_exp, d_row) in enumerate(chips):
        for index in range(2):
            start = columns_of(d_exp, d_row, index, block)
            where = pl.ds(start, block)
            part = nn_dot(near[...], near_weight[:, where]) + nn_dot(far[...], far_weight[:, where])
            here = slice(index * block, (index + 1) * block)
            if chip:
                outs[chip][:, here] = part.astype(BF16)
                continue
            for half in range(2):
                own = slice(half * rows, (half + 1) * rows)
                at = pl.ds(pl.multiple_of((half * 2 + core) * rows, rows), rows)
                outs[0][own, here] = part[own] + residual[at, where].astype(F32)


def own_tokens(rows, n_tokens, core):
    half = rows // 2
    local = lax.broadcasted_iota(jnp.int32, (rows, 1), 0)
    token = local + jnp.where(local >= half, half, 0) + core * half
    lane = lax.broadcasted_iota(jnp.int32, (rows, n_tokens), 1)
    return (lane == token).astype(F32)


def mixed_kernel(count, *refs):
    own, others, (gain, tail, mixed, sent) = refs[0], refs[1:count], refs[count:]
    rows = own.shape[0]
    block = own.shape[1] // 2
    for index in range(2):
        here = slice(index * block, (index + 1) * block)
        total = own[:, here]
        for other in others:
            total = total + other[:, here].astype(F32)
        mixed[:, here] = total
        scale = gain[:, pl.ds(columns_of(0, 0, index, block), block)]
        sent[:rows, here] = (total * scale).astype(BF16)
    sent[rows:, :] = tail[...]


def joined_kernel(*refs):
    out = refs[-1]
    rows = out.shape[0] // (len(refs) - 1)
    for index, ref in enumerate(refs[:-1]):
        out[index * rows : (index + 1) * rows, :] = ref[:rows, :]


def expert_kernel(chips, groups, *refs):
    serves, gain = refs[0], refs[1]
    weights = refs[2:4]
    sents = refs[4 : 4 + len(groups)]
    parts = refs[4 + len(groups) : -1]
    act_ref = refs[-1]
    rows = parts[0].shape[0] // len(groups)
    block = parts[0].shape[1] // 2
    hidden, d_model = weights[0].shape[0] // 2, weights[0].shape[1]
    spots = [
        pl.ds(columns_of(d_exp, d_row, index, block), block)
        for d_exp, d_row in chips
        for index in range(2)
    ]
    part = jnp.concatenate([ref[...] for ref in parts], axis=1)
    weight = jnp.concatenate(
        [
            jnp.concatenate([ref[half * hidden : (half + 1) * hidden, at] for at in spots], axis=1)
            for half in range(2)
            for ref in weights
        ],
        axis=0,
    )
    gates = nt_dot(part, weight)
    gains = jnp.concatenate([gain[:, at] for at in spots], axis=1)
    plain = part.astype(F32)
    squares = jnp.sum(plain * plain * (1.0 / (gains * gains)), axis=1, keepdims=True)
    scale = lax.rsqrt(squares / d_model + 1e-06)
    gate = gates[:, : 2 * hidden] * scale
    up = gates[:, 2 * hidden :] * scale
    act = gate / (1.0 + jnp.exp(-gate)) * up
    lane = lax.broadcasted_iota(jnp.int32, (rows, 2 * rows), 1)
    local = lax.broadcasted_iota(jnp.int32, (rows, 2 * rows), 0)
    chosen = ((lane == local) | (lane == local + rows)).astype(BF16)
    factors = []
    for sent, d_req in zip(sents, groups, strict=True):
        table = nt_dot(chosen, sent[rows:, : 2 * rows])
        factors.append(
            [
                jnp.sum(table * serves[row : row + 1, :], axis=1, keepdims=True)
                for row in (2 * d_req, 2 * d_req + 1)
            ]
        )
    first = jnp.concatenate([pair[0] for pair in factors], axis=0)
    second = jnp.concatenate([pair[1] for pair in factors], axis=0)
    unit = lax.broadcasted_iota(jnp.int32, act.shape, 1)
    act_ref[...] = (act * jnp.where(unit < hidden, first, second)).astype(BF16)


def combine_kernel(count, groups, *refs):
    acts, (near, far), rest = refs[:count], refs[count : count + 2], refs[count + 2 :]
    mixed = None
    if 0 in groups:
        mixed, rest = rest[0], rest[1:]
    rows = acts[0].shape[0] // len(groups)
    total = None
    hidden = near.shape[0] // count
    for index, act in enumerate(acts):
        here = slice(index * hidden, (index + 1) * hidden)
        product = nn_dot(act[...], jnp.concatenate([near[here, :], far[here, :]], axis=0))
        total = product if total is None else total + product
    for index, (d_req, out) in enumerate(zip(groups, rest, strict=True)):
        part = total[index * rows : (index + 1) * rows]
        if d_req == 0:
            part = part + mixed[...]
        out[...] = part.astype(out.dtype)


def summed_kernel(*refs):
    terms, (own_out, other_out) = refs[:-2], refs[-2:]
    _, _, core, _ = place()
    total = terms[0][...]
    for term in terms[1:]:
        total = total + term[...].astype(F32)
    block = total.shape[1] // 2
    own_out[...] = jnp.where(core == 0, total[:, :block], total[:, block:]).astype(BF16)
    other_out[...] = jnp.where(core == 0, total[:, block:], total[:, :block]).astype(BF16)


def final_kernel(own, other, out):
    _, _, core, _ = place()
    rows = own.shape[0] // 2
    for part, place_of in ((own, core), (other, 1 - core)):
        for half in range(2):
            at = pl.ds(pl.multiple_of((half * 2 + place_of) * rows, rows), rows)
            out[at, :] = part[half * rows : (half + 1) * rows, :]


def routes(rows, width, args):
    n_req = lax.axis_size("req")
    n_experts = args[1].shape[0]
    hidden, d_model = args[3].shape
    hbm = pl.BlockSpec(memory_space=pltpu.HBM)
    outs = [
        like((n_experts, width), BF16),
        like((2 * n_req, n_experts), F32),
        like((2 * hidden, d_model), BF16),
    ]
    moves = 2 * hidden * d_model * 2
    return pl.pallas_call(
        lambda *refs: routes_kernel(rows, *refs),
        out_shape=tuple(outs),
        in_specs=[in_smem(), *in_vmem(2), hbm, hbm],
        out_specs=tuple(in_vmem(3)),
        scratch_shapes=[pltpu.SemaphoreType.DMA((2,))],
        cost_estimate=pl.CostEstimate(flops=0, bytes_accessed=moves, transcendentals=0),
        compiler_params=pltpu.CompilerParams(vmem_limit_bytes=VMEM_LIMIT),
        name="routes",
    )(*args[:3], *(pltpu.with_memory_space_constraint(arg, pltpu.HBM) for arg in args[3:]))


def joined_rows(parts, rows=None):
    rows = parts[0].shape[0] if rows is None else rows
    out = like((len(parts) * rows, parts[0].shape[1]), parts[0].dtype)
    return called(joined_kernel, parts, [out], flops=0)[0]


def exchanged(parts, chips):
    return [
        moved(part, 0, 2 * d_row, d_exp) if d_exp or d_row else part
        for part, (d_exp, d_row) in zip(parts, chips, strict=True)
    ]


def spread(value, chips):
    return exchanged([value] * len(chips), chips)


def dense_shards(*args):
    return dense_layer(*args)


def dense_layer(
    queries,
    keys,
    values,
    lengths,
    out_weight,
    residual,
    norm_gain,
    expert_ids,
    gate_weights,
    replica_map,
    w_gate,
    w_up,
    w_down,
):
    n_req, n_kvh, n_exp = (lax.axis_size(axis) for axis in AXES)
    d_model = out_weight.shape[1]
    block = d_model // (n_kvh * n_exp)
    rows = queries.shape[0]
    n_experts = expert_ids.shape[1]
    hidden = w_gate.shape[2]
    chips = [(d_exp, d_row) for d_row in range(n_kvh // 2) for d_exp in range(n_exp)]
    n_chips = len(chips)
    gain = norm_gain.reshape(1, d_model)

    blocks = attention(chips, queries, keys, values, lengths, out_weight, w_down, block)
    down, near_weight, blocks = blocks[5:], blocks[4], list(blocks[:4])
    w_in = (w_gate[0].T, w_up[0].T)
    tail, serves, w_near = routes(rows, 2 * block, (replica_map, expert_ids.T, gate_weights.T, *w_in))
    blocks[3] = moved(blocks[3], 0, 1, 1)
    blocks[1] = moved(blocks[1], 0, 0, 1)
    far_weight = moved(near_weight, 0, 1, 0)
    blocks[2] = moved(blocks[2], 0, 1, 0)
    blocks[3], serves, tail = lax.optimization_barrier((blocks[3], serves, tail))
    wide = (rows, 2 * block)
    sums = called(
        lambda *refs: projection_kernel(chips, *refs),
        (*blocks, near_weight, far_weight, residual),
        [like(wide, F32)] + [like(wide, BF16)] * (n_chips - 1),
        flops=4 * rows * out_weight.size,
        scratch=[pltpu.VMEM((rows, blocks[0].shape[1]), BF16)] * 2,
    )
    later, _ = lax.optimization_barrier((w_near, sums[1]))
    w_far = moved(later, 0, 1, 0)
    down, _ = lax.optimization_barrier((tuple(down), sums[1]))
    sums = exchanged(sums, chips)
    down = exchanged(down, chips)
    down = joined_rows(down)
    down_far = moved(down, 0, 1, 0)
    mixed, sent = called(
        lambda *refs: mixed_kernel(n_chips, *refs),
        (*sums, gain, tail),
        [like(wide, F32), like((rows + n_experts, 2 * block), BF16)],
        flops=8 * rows * block,
    )
    order = range(1, n_req)
    by_group = {0: sent, **{d_req: moved(sent, d_req, 0, 0) for d_req in order}}
    half = n_req // 2
    order = [0, *order]
    terms = {}
    for groups in (tuple(order[:half]), tuple(order[half:])):
        n_rows = len(groups) * rows
        joined = joined_rows([by_group[d_req] for d_req in groups], rows)
        parts = spread(joined, chips)
        (act,) = called(
            lambda *refs, groups=groups: expert_kernel(chips, groups, *refs),
            (serves, gain, w_near, w_far, *(by_group[d_req] for d_req in groups), *parts),
            [like((n_rows, 2 * hidden), BF16)],
            flops=8 * n_rows * d_model * hidden,
        )
        own_mixed = (mixed,) if 0 in groups else ()
        results = called(
            lambda *refs, groups=groups: combine_kernel(n_chips, groups, *refs),
            (*spread(act, chips), down, down_far, *own_mixed),
            [like(wide, F32 if d_req == 0 else BF16) for d_req in groups],
            flops=8 * n_rows * hidden * n_chips * block,
        )
        for d_req, result in zip(groups, results, strict=True):
            terms[d_req] = moved(result, d_req, 0, 0) if d_req else result
    own, other = called(
        summed_kernel,
        [terms[d_req] for d_req in order],
        [like((rows, block), BF16)] * 2,
        flops=4 * n_req * rows * block,
    )
    (out,) = called(
        final_kernel,
        (own, moved(other, 0, 1, 0)),
        [like((2 * rows, block), BF16)],
        flops=4 * rows * block,
    )
    return out


def solution(mesh):
    in_specs = (
        P(("req", "exp"), "kvh"),
        P(("req", "exp"), "kvh", None, None),
        P(("req", "exp"), "kvh", None, None),
        P("req"),
        P(("kvh", "exp"), None),
        P("req", None),
        P(),
        P("req", None),
        P("req", None),
        P(),
        P(("req", "kvh"), None, "exp"),
        P(("req", "kvh"), None, "exp"),
        P(("req", "kvh"), "exp", None),
    )
    out_specs = P("req", ("kvh", "exp"))
    sizes = tuple(mesh.shape[axis] for axis in AXES)

    def run(*args):
        dense = is_dense(sizes, args)
        step = jax.shard_map(
            dense_shards if dense else routed_shards,
            mesh=mesh,
            in_specs=in_specs,
            out_specs=out_specs,
            check_vma=False,
        )
        return step(*args)

    return run
```
